512 devices in a mesh: gx: 8 (over z), gy: 16 (over x_lo, y), gz: 4 (over x_hi, core).
Axes of the slice: x: 4 (x_hi: 2, x_lo: 2; x = x_hi * 2 + x_lo), y: 8, z: 8, core: 2. Of those that a mesh axis runs over, the one named last changes fastest.
Arguments:
- colloc: bfloat16 [12288, 4000], P(('gx', 'gy')), may hold values from -6 to 6
- occ_coeffs: bfloat16 [4000, 1024], P(None, 'gz'), may hold values from -0.09375 to 0.09375
- core: bfloat16 [12288, 16, 768], P('gx', 'gy'), may hold values from -3.9041042e-06 to 3.9041042e-06
Outputs:
- coulomb: float32 [96, 4000], P(('gx', 'gz'), 'gy')
- exchange: float32 [96, 4000], P(('gx', 'gz'), 'gy')
The draws below stay inside these ranges and needn't reach their ends.
All inputs are finite; a program needn't handle non-finite values.
Results may differ from the reference program's by a relative error of at most 0.0089.
Values may be sent and summed in bfloat16 or wider, within the bound.
No kernel may reach another device: no remote copies, remote signals or barrier semaphores. Data moves between devices by JAX's collectives and lax.ppermute only.
A program may use at most 64 MiB of HBM per device.

```python
import jax
import jax.numpy as jnp
from jax import lax

N = 4000
O = 1024
PB = 96
W = 96
P_SIZE = 12288
N_GX = 8
N_GY = 16
N_GZ = 4


def block_levels(rng, extent, cuts, least, top_value):
    def one(position, blocks):
        heights = jax.random.uniform(jax.random.fold_in(jax.random.fold_in(rng, 6), position), (blocks,), jnp.float32, least / len(cuts), top_value / len(cuts))
        return jnp.repeat(jnp.exp(heights), extent[position] // blocks).reshape((-1,) + (1,) * (len(extent) - position - 1))

    loudness = one(*cuts[0])
    for cut in cuts[1:]:
        loudness = loudness * one(*cut)
    return loudness


def scatter_about(stream_key, extent, deviation, reach, pieces=(), kind=jnp.bfloat16):
    values = deviation * jax.random.normal(stream_key, extent, jnp.float32)
    if pieces:
        values = values * block_levels(stream_key, extent, pieces, -0.22, 0.18)
    return jnp.clip(values, -reach, reach).astype(kind)


def setup_inputs(seed: int = 0) -> dict:
    splits = jax.random.split(jax.random.key(seed), 4)
    colloc = scatter_about(splits[0], (P_SIZE, N), 1.0, 6.0, ((0, 128),))
    occ_coeffs = scatter_about(splits[1], (N, O), N ** -0.5, 0.09375, ((1, 4),))
    core = scatter_about(splits[2], (P_SIZE, N_GY, N_GX * PB), (0.008 / (PB * N_GX * N_GY)), 3.904104232788086e-06, ((0, 8), (1, 16)))
    return dict(colloc=colloc, occ_coeffs=occ_coeffs, core=core)


def reference(colloc, occ_coeffs, core):
    zmat = core.reshape(P_SIZE, N_GY, N_GX, PB).transpose(0, 2, 1, 3).reshape(P_SIZE, P_SIZE)
    occ = jnp.dot(colloc, occ_coeffs, preferred_element_type=jnp.float32).astype(jnp.bfloat16)
    density = jnp.sum(jnp.square(occ.astype(jnp.float32)), axis=1).astype(jnp.bfloat16)
    potential = jnp.dot(zmat, density, preferred_element_type=jnp.float32)
    window = colloc[:, :W]
    block_rows = PB * N_GY
    quarter = O // N_GZ

    def add_block(index, acc):
        start = (index * block_rows).astype(jnp.int32)
        occ_rows = lax.dynamic_slice_in_dim(occ, start, block_rows, 0)
        core_rows = lax.dynamic_slice_in_dim(zmat, start, block_rows, 0)
        win_rows = lax.dynamic_slice_in_dim(window, start, block_rows, 0)
        for group in range(N_GZ):
            left = occ_rows[:, group * quarter:(group + 1) * quarter]
            right = occ[:, group * quarter:(group + 1) * quarter]
            gram = jnp.dot(left, right.T, preferred_element_type=jnp.float32)
            mixed = (core_rows.astype(jnp.float32) * gram).astype(jnp.bfloat16)
            acc = acc + jnp.dot(mixed.T, win_rows, preferred_element_type=jnp.float32)
        return acc

    totals = lax.fori_loop(0, N_GX, add_block, jnp.zeros((P_SIZE, W), jnp.float32))
    weighted = (window.astype(jnp.float32) * potential[:, None]).astype(jnp.bfloat16)
    coulomb = jnp.dot(weighted.T, colloc, preferred_element_type=jnp.float32)
    exchange = jnp.dot(totals.astype(jnp.bfloat16).T, colloc, preferred_element_type=jnp.float32)
    return (coulomb, exchange)
```

```python
import jax
import jax.numpy as jnp
from jax import lax
from jax.sharding import Mesh
from jax.sharding import PartitionSpec as P

W = 96
GY = ("gy_0", "gy_1")
GX_GY = ("gx", "gy_0", "gy_1")


def exchange_pieces(pieces, axis):
    return lax.all_to_all(pieces, axis, split_axis=0, concat_axis=0, tiled=True)


def from_everyone(array, axis):
    copies = jnp.broadcast_to(array, (lax.axis_size(axis), *array.shape))
    return exchange_pieces(copies, axis)


def three_pieces(value):
    high = value.astype(jnp.bfloat16)
    rest = value - high.astype(jnp.float32)
    middle = rest.astype(jnp.bfloat16)
    low = (rest - middle.astype(jnp.float32)).astype(jnp.bfloat16)
    return jnp.stack([high, middle, low])


def local(colloc, occ_coeffs, core):
    points, width = colloc.shape
    size_x = lax.axis_size("gx")
    size_y = lax.axis_size(GY)
    size_z = lax.axis_size("gz")
    row_count = core.shape[0]
    flat_cols = core.shape[2]
    col_points = flat_cols // size_x
    per_rows = W // (size_x * size_z)
    own = size_x * per_rows
    core_flat = core.reshape(row_count, flat_cols)

    occ_vals = jnp.dot(colloc, occ_coeffs, preferred_element_type=jnp.float32).astype(jnp.bfloat16)
    window = colloc[:, :W].reshape(points, size_x, size_z, per_rows)
    window = window.transpose(0, 2, 1, 3).reshape(points, W)

    row_vals = from_everyone(jnp.concatenate([occ_vals, window], axis=1), GY)
    col_vals = from_everyone(occ_vals, "gx").reshape(flat_cols, -1)
    row_vals = row_vals.reshape(row_count, -1)
    row_occ = row_vals[:, : occ_vals.shape[1]]
    row_win = row_vals[:, occ_vals.shape[1] :]

    density = jnp.sum(jnp.square(col_vals.astype(jnp.float32)), axis=1).astype(jnp.bfloat16)
    potential_rows = jnp.dot(core_flat, density, preferred_element_type=jnp.float32)
    potential = exchange_pieces(potential_rows.reshape(size_y, points), GY).sum(axis=0)

    gram = lax.dot_general(
        row_occ, col_vals, (((1,), (1,)), ((), ())), preferred_element_type=jnp.float32
    )
    mixed = (core_flat.astype(jnp.float32) * gram).astype(jnp.bfloat16)
    totals = lax.dot_general(
        row_win, mixed, (((0,), (0,)), ((), ())), preferred_element_type=jnp.float32
    ).astype(jnp.bfloat16)
    totals = totals.reshape(size_z, own, size_x, col_points).transpose(2, 0, 1, 3)

    mine = lax.axis_index("gx") == jnp.arange(size_x)
    carried = jnp.where(mine[:, None, None, None], three_pieces(potential)[None, None], 0)
    carried = jnp.broadcast_to(carried, (size_x, size_z, 3, col_points)).astype(jnp.bfloat16)
    sent = jnp.concatenate([totals, carried], axis=2)
    sent = sent.reshape(size_x * size_z, own + 3, col_points)
    owned = exchange_pieces(sent, ("gx", "gz")).astype(jnp.float32).sum(axis=0)

    total_own = owned[:own]
    potential_own = owned[own:].sum(axis=0)
    window_own = lax.dynamic_index_in_dim(
        window.reshape(points, size_z, own), lax.axis_index("gz"), 1, keepdims=False
    )
    weighted = window_own.T.astype(jnp.float32) * potential_own[None, :]
    left = jnp.stack(
        [weighted.reshape(size_x, per_rows, points), total_own.reshape(size_x, per_rows, points)],
        axis=1,
    )
    left = left.reshape(2 * own, points).astype(jnp.bfloat16)
    x_cols = colloc.reshape(points, size_y, width // size_y)
    both = jnp.einsum("mp,pcj->cmj", left, x_cols, preferred_element_type=jnp.float32)
    both = exchange_pieces(both.astype(jnp.bfloat16), GY).astype(jnp.float32).sum(axis=0)
    both = both.astype(jnp.bfloat16).reshape(size_x, 2 * per_rows, width // size_y)
    both = exchange_pieces(both, "gx").astype(jnp.float32).sum(axis=0)
    return (both[:per_rows], both[per_rows:])


def solution(mesh):
    split = Mesh(
        mesh.devices.reshape(mesh.shape["gx"], 2, 8, mesh.shape["gz"]), ("gx", "gy_0", "gy_1", "gz")
    )
    return jax.shard_map(
        local,
        mesh=split,
        in_specs=(P(GX_GY, None), P(None, "gz"), P("gx", GY, None)),
        out_specs=(P(("gx", "gz"), GY), P(("gx", "gz"), GY)),
        check_vma=False,
    )
```

```python
import functools

import jax
import jax.numpy as jnp
from jax import lax
from jax.experimental import pallas as pl
from jax.experimental.pallas import tpu as pltpu
from jax.sharding import Mesh
from jax.sharding import PartitionSpec as P

W = 96
LANES = 128
GRANT = 24 * 1024 * 1024
GY = ("gy_0", "gy_1")
GX_GY = ("gx", "gy_0", "gy_1")
BF16 = jnp.bfloat16
F32 = jnp.float32
IN_VMEM = pl.BlockSpec(memory_space=pltpu.VMEM)
IN_HBM = pl.BlockSpec(memory_space=pl.ANY)
IN_SMEM = pl.BlockSpec(memory_space=pltpu.SMEM)


def exchange_pieces(pieces, axis):
    return lax.all_to_all(pieces, axis, split_axis=0, concat_axis=0, tiled=True)


def one_hot(shape, target):
    rows = lax.broadcasted_iota(jnp.int32, shape, 0)
    cols = lax.broadcasted_iota(jnp.int32, shape, 1)
    return jnp.where(cols == target(rows), 1.0, 0.0).astype(BF16)


def times(left, right, left_dim=1, right_dim=0):
    dims = (((left_dim,), (right_dim,)), ((), ()))
    return lax.dot_general(left, right, dims, preferred_element_type=F32)


def three_pieces(value):
    high = value.astype(BF16).astype(F32)
    middle = (value - high).astype(BF16).astype(F32)
    return high, middle, value - high - middle


def occupied(sizes, chunk, _, colloc_hbm, coeffs_hbm, copies, block, colloc, coeffs, sems):
    size_x, size_z, per_rows = sizes
    width, group = coeffs.shape
    starts = range(0, width, chunk)
    copies_in = []
    for k, at in enumerate(starts):
        part = pl.ds(at, min(chunk, width - at))
        copies_in.append(
            (
                pltpu.make_async_copy(colloc_hbm.at[:, part], colloc.at[:, part], sems.at[0, k]),
                pltpu.make_async_copy(coeffs_hbm.at[part, :], coeffs.at[part, :], sems.at[1, k]),
            )
        )
    for first, second in copies_in:
        first.start()
        second.start()
    acc = jnp.zeros((colloc.shape[0], group), F32)
    for (first, second), at in zip(copies_in, starts):
        first.wait()
        second.wait()
        part = pl.ds(at, min(chunk, width - at))
        acc += times(colloc[:, part], coeffs[part, :])
    occ = acc.astype(BF16)
    for a in range(size_x):
        copies[a] = occ
    own = size_x * per_rows

    def source(col):
        return ((col % own) // per_rows) * (size_z * per_rows) + (col // own) * per_rows + col % per_rows

    pick = one_hot((LANES, LANES), lambda rows: jnp.where(rows < W, source(rows), -1))
    window = times(colloc[:, :LANES], pick, 1, 1)
    block[:, :group] = occ
    block[:, group:] = window.astype(BF16)


def potential_rows(cols, block, core, copies):
    size_x, points, group = cols.shape
    size_y = copies.shape[0]
    vals = cols[...].reshape(size_x * points, group).astype(F32)
    density = jnp.sum(vals * vals, axis=1, keepdims=True).astype(BF16)
    density = jnp.broadcast_to(density, (size_x * points, LANES))
    lane = lax.broadcasted_iota(jnp.int32, (points, LANES), 1)
    occ = block[:, :group]
    window = block[:, group:].astype(F32)
    for c in range(size_y):
        share = times(core[pl.ds(c * points, points), :], density)
        high, middle, low = three_pieces(share)
        tail = jnp.where(lane == W, high, window)
        tail = jnp.where(lane == W + 1, middle, tail)
        tail = jnp.where(lane == W + 2, low, tail)
        copies[c, :, :group] = occ
        copies[c, :, group:] = tail.astype(BF16)


def partial_totals(sizes, per_step, place, rows, cols, core, sent):
    size_x, size_z, per_rows = sizes
    size_y, points, _ = rows.shape
    group = cols.shape[2]
    own = size_x * per_rows
    right = cols[...].reshape(size_x * points, group)
    totals = jnp.zeros((LANES, size_x * points), F32)
    tails = jnp.zeros((points, LANES), F32)
    for c in range(0, size_y, per_step):
        height = per_step * points
        left = rows[pl.ds(c, per_step), :, :group].reshape(height, group)
        tail = rows[pl.ds(c, per_step), :, group:].reshape(height, LANES)
        gram = times(left, right, 1, 1)
        mixed = (core[pl.ds(c * points, height), :].astype(F32) * gram).astype(BF16)
        totals += times(tail, mixed, 0, 0)
        for step in range(per_step):
            tails += tail[step * points : (step + 1) * points].astype(F32)
    lane = lax.broadcasted_iota(jnp.int32, (points, LANES), 1)
    share = jnp.sum(jnp.where(lane < W, 0.0, tails), axis=1, keepdims=True)
    high, middle, low = three_pieces(share)
    pieces = jnp.where(lane == 0, high, jnp.where(lane == 1, middle, jnp.where(lane == 2, low, 0.0)))
    square = one_hot((points, points), lambda rows: rows)
    pieces = times(pieces.astype(BF16), square, 0, 0)[: sent.shape[1] - own]
    for a in range(size_x):
        carried = jnp.where(place[0] == a, pieces, 0.0).astype(BF16)
        for g in range(size_z):
            part = totals[g * own : (g + 1) * own, a * points : (a + 1) * points]
            sent[a * size_z + g, :own] = part.astype(BF16)
            sent[a * size_z + g, own:] = carried


def final_shares(sizes, place, arrived, block, colloc, shares, rows):
    size_x, size_z, per_rows = sizes
    size_y, height, part = shares.shape
    own = size_x * per_rows
    total = jnp.sum(arrived[...].astype(F32), axis=0)
    potential = jnp.sum(total[own:], axis=0, keepdims=True)
    window = block[:, block.shape[1] - LANES :]
    pick = one_hot((own, LANES), lambda row: row + place[1] * own)
    weighted = (times(pick, window, 1, 1) * potential).astype(BF16)

    def spread(which):
        def target(row):
            inside = row % (2 * per_rows)
            found = (row // (2 * per_rows)) * per_rows + inside % per_rows
            return jnp.where(inside // per_rows == which, found, -1)

        return one_hot((height, own), target)

    left = times(spread(0), weighted) + times(spread(1), total[:own].astype(BF16))
    rows[:, : colloc.shape[1]] = times(left.astype(BF16), colloc[...])
    for c in range(size_y):
        start = (c * part) // LANES * LANES
        span = -(-(c * part + part - start) // LANES) * LANES
        found = rows[:, pl.ds(start, span)]
        shift = c * part - start
        if shift:
            found = pltpu.roll(found, span - shift, 1)
        shares[c] = found[:, :part].astype(BF16)


def local(colloc, occ_coeffs, core):
    points, width = colloc.shape
    group = occ_coeffs.shape[1]
    size_x = lax.axis_size("gx")
    size_y = lax.axis_size(GY)
    size_z = lax.axis_size("gz")
    row_count = core.shape[0]
    flat_cols = core.shape[2]
    per_rows = W // (size_x * size_z)
    own = size_x * per_rows
    part = width // size_y
    sizes = (size_x, size_z, per_rows)
    core_flat = core.reshape(row_count, flat_cols)
    place = jnp.stack([lax.axis_index("gx"), lax.axis_index("gz")]).astype(jnp.int32)
    chunk = 8 * LANES
    steps = -(-width // chunk)

    copies, block = pl.pallas_call(
        functools.partial(occupied, sizes, chunk),
        in_specs=[IN_SMEM, IN_HBM, IN_HBM],
        out_specs=[IN_VMEM, IN_VMEM],
        out_shape=[
            jax.ShapeDtypeStruct((size_x, points, group), BF16),
            jax.ShapeDtypeStruct((points, group + LANES), BF16),
        ],
        scratch_shapes=[
            pltpu.VMEM((points, width), BF16),
            pltpu.VMEM((width, group), BF16),
            pltpu.SemaphoreType.DMA((2, steps)),
        ],
        compiler_params=pltpu.CompilerParams(vmem_limit_bytes=GRANT),
        name="occupied",
    )(place, colloc, occ_coeffs)
    cols = exchange_pieces(copies, "gx")

    row_copies = pl.pallas_call(
        potential_rows,
        in_specs=[IN_VMEM, IN_VMEM, IN_VMEM],
        out_specs=IN_VMEM,
        out_shape=jax.ShapeDtypeStruct((size_y, points, group + LANES), BF16),
        compiler_params=pltpu.CompilerParams(vmem_limit_bytes=GRANT),
        name="potential_rows",
    )(cols, block, core_flat)
    rows = exchange_pieces(row_copies, GY)

    sent = pl.pallas_call(
        functools.partial(partial_totals, sizes, 4),
        in_specs=[IN_SMEM, IN_VMEM, IN_VMEM, IN_VMEM],
        out_specs=IN_VMEM,
        out_shape=jax.ShapeDtypeStruct((size_x * size_z, own + 8, points), BF16),
        compiler_params=pltpu.CompilerParams(vmem_limit_bytes=GRANT),
        name="partial_totals",
    )(place, rows, cols, core_flat)
    arrived = exchange_pieces(sent, ("gx", "gz"))

    shares = pl.pallas_call(
        functools.partial(final_shares, sizes),
        in_specs=[IN_SMEM, IN_VMEM, IN_VMEM, IN_VMEM],
        out_specs=IN_VMEM,
        out_shape=jax.ShapeDtypeStruct((size_y, 2 * own, part), BF16),
        scratch_shapes=[pltpu.VMEM((2 * own, -(-width // LANES) * LANES), F32)],
        compiler_params=pltpu.CompilerParams(vmem_limit_bytes=GRANT),
        name="final_shares",
    )(place, arrived, block, colloc)
    both = exchange_pieces(shares, GY).astype(F32).sum(axis=0)
    both = both.astype(BF16).reshape(size_x, 2 * per_rows, part)
    both = exchange_pieces(both, "gx").astype(F32).sum(axis=0)
    return (both[:per_rows], both[per_rows:])


def solution(mesh):
    split = Mesh(
        mesh.devices.reshape(mesh.shape["gx"], 2, 8, mesh.shape["gz"]), ("gx", "gy_0", "gy_1", "gz")
    )
    return jax.shard_map(
        local,
        mesh=split,
        in_specs=(P(GX_GY, None), P(None, "gz"), P("gx", GY, None)),
        out_specs=(P(("gx", "gz"), GY), P(("gx", "gz"), GY)),
        check_vma=False,
    )
```

```python
import functools

import jax
import jax.numpy as jnp
from jax import lax
from jax.experimental import pallas as pl
from jax.experimental.pallas import tpu as pltpu
from jax.sharding import Mesh
from jax.sharding import PartitionSpec as P

W = 96
LANES = 128
GRANT = 24 * 1024 * 1024
GY = ("gy_0", "gy_1")
GX_GY = ("gx", "gy_0", "gy_1")
BF16 = jnp.bfloat16
F32 = jnp.float32
IN_VMEM = pl.BlockSpec(memory_space=pltpu.VMEM)
IN_HBM = pl.BlockSpec(memory_space=pltpu.HBM)
IN_SMEM = pl.BlockSpec(memory_space=pltpu.SMEM)
PARAMS = pltpu.CompilerParams(vmem_limit_bytes=GRANT)


def exchange_pieces(pieces, axis):
    return lax.all_to_all(pieces, axis, split_axis=0, concat_axis=0, tiled=True)


def one_hot(shape, target):
    rows = lax.broadcasted_iota(jnp.int32, shape, 0)
    cols = lax.broadcasted_iota(jnp.int32, shape, 1)
    return jnp.where(cols == target(rows), 1.0, 0.0).astype(BF16)


def times(left, right, left_dim=1, right_dim=0):
    dims = (((left_dim,), (right_dim,)), ((), ()))
    return lax.dot_general(left, right, dims, preferred_element_type=F32)


def three_pieces(value):
    high = value.astype(BF16).astype(F32)
    middle = (value - high).astype(BF16).astype(F32)
    return high, middle, value - high - middle


def occupied(sizes, chunk, _, colloc_hbm, coeffs_hbm, copies, block, sums, colloc, coeffs, sems):
    size_x, size_z, per_rows = sizes
    width, group = coeffs.shape
    points = colloc.shape[0]
    starts = range(0, width, chunk)
    copies_in = []
    for k, at in enumerate(starts):
        part = pl.ds(at, min(chunk, width - at))
        copies_in.append(
            (
                pltpu.make_async_copy(colloc_hbm.at[:, part], colloc.at[:, part], sems.at[0, k]),
                pltpu.make_async_copy(coeffs_hbm.at[part, :], coeffs.at[part, :], sems.at[1, k]),
            )
        )
    for first, second in copies_in:
        first.start()
        second.start()
    acc = jnp.zeros((points, group), F32)
    for (first, second), at in zip(copies_in, starts):
        first.wait()
        second.wait()
        part = pl.ds(at, min(chunk, width - at))
        acc += times(colloc[:, part], coeffs[part, :])
    occ = acc.astype(BF16)
    vals = occ.astype(F32)
    density = jnp.sum(vals * vals, axis=1, keepdims=True).astype(BF16)
    square = one_hot((points, points), lambda rows: rows)
    density = times(jnp.broadcast_to(density, (points, LANES)), square, 0, 0)[: sums.shape[1]]
    own = size_x * per_rows

    def source(col):
        return ((col % own) // per_rows) * (size_z * per_rows) + (col // own) * per_rows + col % per_rows

    pick = one_hot((LANES, LANES), lambda rows: jnp.where(rows < W, source(rows), -1))
    window = times(colloc[:, :LANES], pick, 1, 1)
    block[:, :group] = occ
    block[:, group:] = window.astype(BF16)
    for a in range(size_x):
        sums[a] = density
        copies[a] = occ


def potential_rows(sums, block, core, copies, density):
    size_x, _, points = sums.shape
    size_y = copies.shape[0]
    group = block.shape[1] - LANES
    for a in range(size_x):
        density[:, a * points : (a + 1) * points] = sums[a]
    right = jnp.broadcast_to(density[:1, :], (LANES, size_x * points)).astype(BF16)
    lane = lax.broadcasted_iota(jnp.int32, (points, LANES), 1)
    occ = block[:, :group]
    window = block[:, group:].astype(F32)
    halves = core.shape[0] // (size_y * points)
    for y in range(size_y):
        tail = window
        for half in range(halves):
            share = times(core[pl.ds((half * size_y + y) * points, points), :], right, 1, 1)
            for k, piece in enumerate(three_pieces(share)):
                tail = jnp.where(lane == W + 3 * half + k, piece, tail)
        copies[y, :, :group] = occ
        copies[y, :, group:] = tail.astype(BF16)


def add_rows(per_step, rows, half, right, core, totals, tails):
    size_y, points, _ = rows.shape
    group = right.shape[1]
    height = per_step * points
    for y in range(0, size_y, per_step):
        left = rows[pl.ds(y, per_step), :, :group].reshape(height, group)
        tail = rows[pl.ds(y, per_step), :, group:].reshape(height, LANES)
        gram = times(left, right, 1, 1)
        at = pl.multiple_of(half * (size_y * points) + y * points, points)
        mixed = (core[pl.ds(at, height), :].astype(F32) * gram).astype(BF16)
        totals += times(tail, mixed, 0, 0)
        for step in range(per_step):
            tails += tail[step * points : (step + 1) * points].astype(F32)
    return totals, tails


def near_totals(per_step, place, near, cols, core, totals, tails):
    right = cols[...].reshape(-1, cols.shape[2])
    zeros = (jnp.zeros(totals.shape, F32), jnp.zeros(tails.shape, F32))
    totals[...], tails[...] = add_rows(per_step, near, place[2], right, core, *zeros)


def partial_totals(sizes, per_step, place, totals, tails, far, cols, core, sent, stored):
    size_x, size_z, per_rows = sizes
    points = far.shape[1]
    own = size_x * per_rows
    right = cols[...].reshape(-1, cols.shape[2])
    totals, tails = add_rows(per_step, far, 1 - place[2], right, core, totals[...], tails[...])
    lane = lax.broadcasted_iota(jnp.int32, (points, LANES), 1)
    first = W + 3 * place[2]
    kept = (lane >= first) & (lane < first + 3)
    share = jnp.sum(jnp.where(kept, tails, 0.0), axis=1, keepdims=True)
    per_row = points // own
    point = lax.broadcasted_iota(jnp.int32, (points, LANES), 0)
    behind = W + 3 * (point % per_row)
    packed = jnp.zeros((points, LANES), F32)
    for k, piece in enumerate(three_pieces(share)):
        packed = jnp.where(lane == behind + k, piece, packed)
    fold_row = lax.broadcasted_iota(jnp.int32, (own, points), 0)
    fold_col = lax.broadcasted_iota(jnp.int32, (own, points), 1)
    fold = jnp.where(fold_col // per_row == fold_row, 1.0, 0.0).astype(BF16)
    packed = times(fold, packed.astype(BF16))
    stored[:, : size_x * points] = totals
    lane = lax.broadcasted_iota(jnp.int32, (LANES, LANES), 1)
    for a in range(size_x):
        start = a * points // LANES * LANES
        shift = a * points - start
        found = stored[:, pl.ds(start, 2 * LANES)]
        if shift:
            found = pltpu.roll(found, 2 * LANES - shift, 1)
        found = jnp.where(lane < points, found[:, :LANES], 0.0)
        carried = jnp.where(place[0] == a, packed, 0.0)
        for g in range(size_z):
            sent[a * size_z + g] = (found[g * own : (g + 1) * own] + carried).astype(BF16)


def final_shares(sizes, place, arrived, block, colloc, shares, rows):
    size_x, _, per_rows = sizes
    size_y, height, part = shares.shape
    points = block.shape[0]
    own = size_x * per_rows
    per_row = points // own
    total = jnp.sum(arrived[...].astype(F32), axis=0)
    unfold_row = lax.broadcasted_iota(jnp.int32, (points, own), 0)
    unfold_col = lax.broadcasted_iota(jnp.int32, (points, own), 1)
    unfold = jnp.where(unfold_row // per_row == unfold_col, 1.0, 0.0).astype(BF16)
    spread_out = jnp.zeros((points, LANES), F32)
    for piece in three_pieces(total):
        spread_out += times(unfold, piece.astype(BF16))
    lane = lax.broadcasted_iota(jnp.int32, (points, LANES), 1)
    behind = W + 3 * (lax.broadcasted_iota(jnp.int32, (points, LANES), 0) % per_row)
    kept = (lane >= behind) & (lane < behind + 3)
    potential = jnp.sum(jnp.where(kept, spread_out, 0.0), axis=1, keepdims=True)
    window = block[:, block.shape[1] - LANES :]
    pick = one_hot((own, LANES), lambda row: row + place[1] * own)
    weighted = (times(window, pick, 1, 1) * potential).astype(BF16)

    def spread(which):
        def target(row):
            inside = row % (2 * per_rows)
            found = (row // (2 * per_rows)) * per_rows + inside % per_rows
            return jnp.where(inside // per_rows == which, found, -1)

        return one_hot((height, own), target)

    left = times(spread(0), weighted, 1, 1) + times(spread(1), total[:, :points].astype(BF16))
    rows[:, : colloc.shape[1]] = times(left.astype(BF16), colloc[...])
    for c in range(size_y):
        start = (c * part) // LANES * LANES
        span = -(-(c * part + part - start) // LANES) * LANES
        found = rows[:, pl.ds(start, span)]
        shift = c * part - start
        if shift:
            found = pltpu.roll(found, span - shift, 1)
        shares[c] = found[:, :part].astype(BF16)


def work(colloc, occ_coeffs, core):
    points, width = colloc.shape
    group = occ_coeffs.shape[1]
    size_x = lax.axis_size("gx")
    near_y = lax.axis_size("gy_1")
    size_y = lax.axis_size(GY)
    size_z = lax.axis_size("gz")
    row_count = core.shape[0]
    flat_cols = core.shape[2]
    per_rows = W // (size_x * size_z)
    own = size_x * per_rows
    part = width // size_y
    sizes = (size_x, size_z, per_rows)
    core_flat = core.reshape(row_count, flat_cols)
    place = jnp.stack([lax.axis_index("gx"), lax.axis_index("gz"), lax.axis_index("gy_0")])
    place = place.astype(jnp.int32)
    chunk = 8 * LANES
    steps = -(-width // chunk)

    copies, block, sums = pl.pallas_call(
        functools.partial(occupied, sizes, chunk),
        in_specs=[IN_SMEM, IN_HBM, IN_HBM],
        out_specs=[IN_VMEM, IN_VMEM, IN_VMEM],
        out_shape=[
            jax.ShapeDtypeStruct((size_x, points, group), BF16),
            jax.ShapeDtypeStruct((points, group + LANES), BF16),
            jax.ShapeDtypeStruct((size_x, 8, points), F32),
        ],
        scratch_shapes=[
            pltpu.VMEM((points, width), BF16),
            pltpu.VMEM((width, group), BF16),
            pltpu.SemaphoreType.DMA((2, steps)),
        ],
        compiler_params=pltpu.CompilerParams(vmem_limit_bytes=53 * 1024 * 1024),
        name="occupied",
    )(place, colloc, occ_coeffs)
    sums = exchange_pieces(sums, "gx")

    row_copies = pl.pallas_call(
        potential_rows,
        in_specs=[IN_VMEM, IN_VMEM, IN_VMEM],
        out_specs=IN_VMEM,
        out_shape=jax.ShapeDtypeStruct((near_y, points, group + LANES), BF16),
        scratch_shapes=[pltpu.VMEM((8, flat_cols), F32)],
        compiler_params=PARAMS,
        name="potential_rows",
    )(sums, block, core_flat)
    near = exchange_pieces(row_copies, "gy_1")
    far = lax.ppermute(near, "gy_0", [(0, 1), (1, 0)])
    cols = exchange_pieces(copies, "gx")

    totals, tails = pl.pallas_call(
        functools.partial(near_totals, 4),
        in_specs=[IN_SMEM, IN_VMEM, IN_VMEM, IN_VMEM],
        out_specs=[IN_VMEM, IN_VMEM],
        out_shape=[
            jax.ShapeDtypeStruct((LANES, flat_cols), F32),
            jax.ShapeDtypeStruct((points, LANES), F32),
        ],
        compiler_params=PARAMS,
        name="near_totals",
    )(place, near, cols, core_flat)
    sent = pl.pallas_call(
        functools.partial(partial_totals, sizes, 4),
        in_specs=[IN_SMEM, IN_VMEM, IN_VMEM, IN_VMEM, IN_VMEM, IN_VMEM],
        out_specs=IN_VMEM,
        out_shape=jax.ShapeDtypeStruct((size_x * size_z, own, LANES), BF16),
        scratch_shapes=[pltpu.VMEM((LANES, flat_cols + LANES), F32)],
        compiler_params=PARAMS,
        name="partial_totals",
    )(place, totals, tails, far, cols, core_flat)
    arrived = exchange_pieces(sent, ("gx", "gz"))

    shares = pl.pallas_call(
        functools.partial(final_shares, sizes),
        in_specs=[IN_SMEM, IN_VMEM, IN_VMEM, IN_VMEM],
        out_specs=IN_VMEM,
        out_shape=jax.ShapeDtypeStruct((size_y, 2 * own, part), BF16),
        scratch_shapes=[pltpu.VMEM((2 * own, -(-width // LANES) * LANES), F32)],
        compiler_params=PARAMS,
        name="final_shares",
    )(place, arrived, block, colloc)
    both = exchange_pieces(shares, GY).astype(F32).sum(axis=0)
    both = both.astype(BF16).reshape(size_x, 2 * per_rows, part)
    both = exchange_pieces(both, "gx").astype(F32).sum(axis=0)
    return (both[:per_rows], both[per_rows:])


def solution(mesh):
    split = Mesh(
        mesh.devices.reshape(mesh.shape["gx"], 2, 8, mesh.shape["gz"]), ("gx", "gy_0", "gy_1", "gz")
    )
    return jax.shard_map(
        work,
        mesh=split,
        in_specs=(P(GX_GY, None), P(None, "gz"), P("gx", GY, None)),
        out_specs=(P(("gx", "gz"), GY), P(("gx", "gz"), GY)),
        check_vma=False,
    )
```

```python
import functools

import jax
import jax.numpy as jnp
from jax import lax
from jax.experimental import pallas as pl
from jax.experimental.pallas import tpu as pltpu
from jax.sharding import Mesh
from jax.sharding import PartitionSpec as P

W = 96
LANES = 128
SUBLANES = 8
GRANT = 24 * 1024 * 1024
GY = ("gy_0", "gy_1")
GX_GY = ("gx", "gy_0", "gy_1")
BF16 = jnp.bfloat16
F32 = jnp.float32
IN_VMEM = pl.BlockSpec(memory_space=pltpu.VMEM)
IN_HBM = pl.BlockSpec(memory_space=pltpu.HBM)
IN_SMEM = pl.BlockSpec(memory_space=pltpu.SMEM)
PARAMS = pltpu.CompilerParams(vmem_limit_bytes=GRANT)


def exchange_pieces(pieces, axis):
    return lax.all_to_all(pieces, axis, split_axis=0, concat_axis=0, tiled=True)


def one_hot(shape, target):
    rows = lax.broadcasted_iota(jnp.int32, shape, 0)
    cols = lax.broadcasted_iota(jnp.int32, shape, 1)
    return jnp.where(cols == target(rows), 1.0, 0.0).astype(BF16)


def times(left, right, left_dim=1, right_dim=0):
    dims = (((left_dim,), (right_dim,)), ((), ()))
    return lax.dot_general(left, right, dims, preferred_element_type=F32)


def three_pieces(value):
    high = value.astype(BF16).astype(F32)
    middle = (value - high).astype(BF16).astype(F32)
    return high, middle, value - high - middle


def occupied(sizes, chunk, _, colloc_hbm, coeffs_hbm, copies, block, sums, colloc, coeffs, sems):
    size_x, size_z, per_rows = sizes
    width, group = coeffs.shape
    points = colloc.shape[0]
    starts = range(0, width, chunk)
    copies_in = []
    for k, at in enumerate(starts):
        part = pl.ds(at, min(chunk, width - at))
        copies_in.append(
            (
                pltpu.make_async_copy(colloc_hbm.at[:, part], colloc.at[:, part], sems.at[0, k]),
                pltpu.make_async_copy(coeffs_hbm.at[part, :], coeffs.at[part, :], sems.at[1, k]),
            )
        )
    for first, second in copies_in:
        first.start()
        second.start()
    acc = jnp.zeros((points, group), F32)
    for (first, second), at in zip(copies_in, starts):
        first.wait()
        second.wait()
        part = pl.ds(at, min(chunk, width - at))
        acc += times(colloc[:, part], coeffs[part, :])
    occ = acc.astype(BF16)
    vals = occ.astype(F32)
    density = jnp.sum(vals * vals, axis=1, keepdims=True).astype(BF16)
    square = one_hot((points, points), lambda rows: rows)
    density = times(jnp.broadcast_to(density, (points, LANES)), square, 0, 0)[: sums.shape[1]]
    own = size_x * per_rows

    def source(col):
        return ((col % own) // per_rows) * (size_z * per_rows) + (col // own) * per_rows + col % per_rows

    pick = one_hot((LANES, LANES), lambda rows: jnp.where(rows < W, source(rows), -1))
    window = times(colloc[:, :LANES], pick, 1, 1)
    block[:, :group] = occ
    block[:, group:] = window.astype(BF16)
    for a in range(size_x):
        sums[a] = density
        copies[a] = occ


def potential_rows(sums, block, core, copies, density):
    size_x, _, points = sums.shape
    size_y = copies.shape[0]
    group = block.shape[1] - LANES
    for a in range(size_x):
        density[:, a * points : (a + 1) * points] = sums[a]
    right = jnp.broadcast_to(density[:1, :], (LANES, size_x * points)).astype(BF16)
    lane = lax.broadcasted_iota(jnp.int32, (points, LANES), 1)
    occ = block[:, :group]
    window = block[:, group:].astype(F32)
    halves = core.shape[0] // (size_y * points)
    for y in range(size_y):
        tail = window
        for half in range(halves):
            share = times(core[pl.ds((half * size_y + y) * points, points), :], right, 1, 1)
            for k, piece in enumerate(three_pieces(share)):
                tail = jnp.where(lane == W + 3 * half + k, piece, tail)
        copies[y, :, :group] = occ
        copies[y, :, group:] = tail.astype(BF16)


def add_rows(per_step, rows, half, right, core, totals, tails):
    size_y, points, _ = rows.shape
    group = right.shape[1]
    height = per_step * points
    for y in range(0, size_y, per_step):
        left = rows[pl.ds(y, per_step), :, :group].reshape(height, group)
        tail = rows[pl.ds(y, per_step), :, group:].reshape(height, LANES)
        gram = times(left, right, 1, 1)
        at = pl.multiple_of(half * (size_y * points) + y * points, points)
        mixed = (core[pl.ds(at, height), :].astype(F32) * gram).astype(BF16)
        totals += times(tail, mixed, 0, 0)
        for step in range(per_step):
            tails += tail[step * points : (step + 1) * points].astype(F32)
    return totals, tails


def near_totals(per_step, place, near, cols, core, totals, tails):
    right = cols[...].reshape(-1, cols.shape[2])
    zeros = (jnp.zeros(totals.shape, F32), jnp.zeros(tails.shape, F32))
    totals[...], tails[...] = add_rows(per_step, near, place[2], right, core, *zeros)


def partial_totals(sizes, per_step, place, totals, tails, far, cols, core, sent, stored):
    size_x, size_z, per_rows = sizes
    points = far.shape[1]
    own = size_x * per_rows
    right = cols[...].reshape(-1, cols.shape[2])
    totals, tails = add_rows(per_step, far, 1 - place[2], right, core, totals[...], tails[...])
    lane = lax.broadcasted_iota(jnp.int32, (points, LANES), 1)
    first = W + 3 * place[2]
    kept = (lane >= first) & (lane < first + 3)
    share = jnp.sum(jnp.where(kept, tails, 0.0), axis=1, keepdims=True)
    per_row = points // own
    point = lax.broadcasted_iota(jnp.int32, (points, LANES), 0)
    behind = W + 3 * (point % per_row)
    packed = jnp.zeros((points, LANES), F32)
    for k, piece in enumerate(three_pieces(share)):
        packed = jnp.where(lane == behind + k, piece, packed)
    fold_row = lax.broadcasted_iota(jnp.int32, (own, points), 0)
    fold_col = lax.broadcasted_iota(jnp.int32, (own, points), 1)
    fold = jnp.where(fold_col // per_row == fold_row, 1.0, 0.0).astype(BF16)
    packed = times(fold, packed.astype(BF16))
    stored[:, : size_x * points] = totals
    lane = lax.broadcasted_iota(jnp.int32, (LANES, LANES), 1)
    for a in range(size_x):
        start = a * points // LANES * LANES
        shift = a * points - start
        found = stored[:, pl.ds(start, 2 * LANES)]
        if shift:
            found = pltpu.roll(found, 2 * LANES - shift, 1)
        found = jnp.where(lane < points, found[:, :LANES], 0.0)
        carried = jnp.where(place[0] == a, packed, 0.0)
        for g in range(size_z):
            sent[a * size_z + g] = (found[g * own : (g + 1) * own] + carried).astype(BF16)


def final_shares(sizes, place, arrived, block, colloc, shares, rows):
    size_x, _, per_rows = sizes
    pieces, pair, part = shares.shape
    size_y = pieces // size_x
    points = block.shape[0]
    own = size_x * per_rows
    per_row = points // own
    total = jnp.sum(arrived[...].astype(F32), axis=0)
    unfold_row = lax.broadcasted_iota(jnp.int32, (points, own), 0)
    unfold_col = lax.broadcasted_iota(jnp.int32, (points, own), 1)
    unfold = jnp.where(unfold_row // per_row == unfold_col, 1.0, 0.0).astype(BF16)
    spread_out = jnp.zeros((points, LANES), F32)
    for piece in three_pieces(total):
        spread_out += times(unfold, piece.astype(BF16))
    lane = lax.broadcasted_iota(jnp.int32, (points, LANES), 1)
    behind = W + 3 * (lax.broadcasted_iota(jnp.int32, (points, LANES), 0) % per_row)
    kept = (lane >= behind) & (lane < behind + 3)
    potential = jnp.sum(jnp.where(kept, spread_out, 0.0), axis=1, keepdims=True)
    window = block[:, block.shape[1] - LANES :]
    pick = one_hot((own, LANES), lambda row: row + place[1] * own)
    weighted = (times(window, pick, 1, 1) * potential).astype(BF16)

    def spread(which):
        def target(row):
            inside = row % SUBLANES
            found = (row // SUBLANES) * per_rows + inside % per_rows
            return jnp.where(inside // per_rows == which, found, -1)

        return one_hot((size_x * SUBLANES, own), target)

    left = times(spread(0), weighted, 1, 1) + times(spread(1), total[:, :points].astype(BF16))
    rows[:, : colloc.shape[1]] = times(left.astype(BF16), colloc[...])
    for c in range(size_y):
        start = (c * part) // LANES * LANES
        span = -(-(c * part + part - start) // LANES) * LANES
        found = rows[:, pl.ds(start, span)]
        shift = c * part - start
        if shift:
            found = pltpu.roll(found, span - shift, 1)
        for a in range(size_x):
            at = a * SUBLANES
            shares[a * size_y + c] = found[at : at + pair, :part].astype(BF16)


def outputs(arrived, coulomb, exchange):
    per_rows = coulomb.shape[0]
    total = jnp.sum(arrived[...].astype(F32), axis=0)
    coulomb[...] = total[:per_rows]
    exchange[...] = total[per_rows:]


def work(colloc, occ_coeffs, core):
    points, width = colloc.shape
    group = occ_coeffs.shape[1]
    size_x = lax.axis_size("gx")
    near_y = lax.axis_size("gy_1")
    size_y = lax.axis_size(GY)
    size_z = lax.axis_size("gz")
    row_count = core.shape[0]
    flat_cols = core.shape[2]
    per_rows = W // (size_x * size_z)
    own = size_x * per_rows
    part = width // size_y
    sizes = (size_x, size_z, per_rows)
    core_flat = core.reshape(row_count, flat_cols)
    place = jnp.stack([lax.axis_index("gx"), lax.axis_index("gz"), lax.axis_index("gy_0")])
    place = place.astype(jnp.int32)
    chunk = 8 * LANES
    steps = -(-width // chunk)

    copies, block, sums = pl.pallas_call(
        functools.partial(occupied, sizes, chunk),
        in_specs=[IN_SMEM, IN_HBM, IN_HBM],
        out_specs=[IN_VMEM, IN_VMEM, IN_VMEM],
        out_shape=[
            jax.ShapeDtypeStruct((size_x, points, group), BF16),
            jax.ShapeDtypeStruct((points, group + LANES), BF16),
            jax.ShapeDtypeStruct((size_x, 8, points), F32),
        ],
        scratch_shapes=[
            pltpu.VMEM((points, width), BF16),
            pltpu.VMEM((width, group), BF16),
            pltpu.SemaphoreType.DMA((2, steps)),
        ],
        compiler_params=pltpu.CompilerParams(vmem_limit_bytes=53 * 1024 * 1024),
        name="occupied",
    )(place, colloc, occ_coeffs)
    sums = exchange_pieces(sums, "gx")

    row_copies = pl.pallas_call(
        potential_rows,
        in_specs=[IN_VMEM, IN_VMEM, IN_VMEM],
        out_specs=IN_VMEM,
        out_shape=jax.ShapeDtypeStruct((near_y, points, group + LANES), BF16),
        scratch_shapes=[pltpu.VMEM((8, flat_cols), F32)],
        compiler_params=PARAMS,
        name="potential_rows",
    )(sums, block, core_flat)
    near = exchange_pieces(row_copies, "gy_1")
    far = lax.ppermute(near, "gy_0", [(0, 1), (1, 0)])
    cols = exchange_pieces(copies, "gx")

    totals, tails = pl.pallas_call(
        functools.partial(near_totals, 4),
        in_specs=[IN_SMEM, IN_VMEM, IN_VMEM, IN_VMEM],
        out_specs=[IN_VMEM, IN_VMEM],
        out_shape=[
            jax.ShapeDtypeStruct((LANES, flat_cols), F32),
            jax.ShapeDtypeStruct((points, LANES), F32),
        ],
        compiler_params=PARAMS,
        name="near_totals",
    )(place, near, cols, core_flat)
    sent = pl.pallas_call(
        functools.partial(partial_totals, sizes, 4),
        in_specs=[IN_SMEM, IN_VMEM, IN_VMEM, IN_VMEM, IN_VMEM, IN_VMEM],
        out_specs=IN_VMEM,
        out_shape=jax.ShapeDtypeStruct((size_x * size_z, own, LANES), BF16),
        scratch_shapes=[pltpu.VMEM((LANES, flat_cols + LANES), F32)],
        compiler_params=PARAMS,
        name="partial_totals",
    )(place, totals, tails, far, cols, core_flat)
    arrived = exchange_pieces(sent, ("gx", "gz"))

    shares = pl.pallas_call(
        functools.partial(final_shares, sizes),
        in_specs=[IN_SMEM, IN_VMEM, IN_VMEM, IN_VMEM],
        out_specs=IN_VMEM,
        out_shape=jax.ShapeDtypeStruct((size_x * size_y, 2 * per_rows, part), BF16),
        scratch_shapes=[pltpu.VMEM((size_x * SUBLANES, -(-width // LANES) * LANES), F32)],
        compiler_params=PARAMS,
        name="final_shares",
    )(place, arrived, block, colloc)
    arrived = exchange_pieces(shares, GX_GY)
    return pl.pallas_call(
        outputs,
        in_specs=[IN_VMEM],
        out_specs=[IN_VMEM, IN_VMEM],
        out_shape=[jax.ShapeDtypeStruct((per_rows, part), F32)] * 2,
        compiler_params=PARAMS,
        name="outputs",
    )(arrived)


def solution(mesh):
    split = Mesh(
        mesh.devices.reshape(mesh.shape["gx"], 2, 8, mesh.shape["gz"]), ("gx", "gy_0", "gy_1", "gz")
    )
    return jax.shard_map(
        work,
        mesh=split,
        in_specs=(P(GX_GY, None), P(None, "gz"), P("gx", GY, None)),
        out_specs=(P(("gx", "gz"), GY), P(("gx", "gz"), GY)),
        check_vma=False,
    )
```

```python
import functools

import jax
import jax.numpy as jnp
from jax import lax
from jax.experimental import pallas as pl
from jax.experimental.pallas import tpu as pltpu
from jax.sharding import Mesh
from jax.sharding import PartitionSpec as P

W = 96
LANES = 128
SUBLANES = 8
GRANT = 24 * 1024 * 1024
GY = ("gy_0", "gy_1")
GX_GY = ("gx", "gy_0", "gy_1")
BF16 = jnp.bfloat16
F32 = jnp.float32
IN_VMEM = pl.BlockSpec(memory_space=pltpu.VMEM)
IN_HBM = pl.BlockSpec(memory_space=pltpu.HBM)
IN_SMEM = pl.BlockSpec(memory_space=pltpu.SMEM)
PARAMS = pltpu.CompilerParams(vmem_limit_bytes=GRANT)


def exchange_pieces(pieces, axis):
    return lax.all_to_all(pieces, axis, split_axis=0, concat_axis=0, tiled=True)


def one_hot(shape, target):
    rows = lax.broadcasted_iota(jnp.int32, shape, 0)
    cols = lax.broadcasted_iota(jnp.int32, shape, 1)
    return jnp.where(cols == target(rows), 1.0, 0.0).astype(BF16)


def times(left, right, left_dim=1, right_dim=0):
    dims = (((left_dim,), (right_dim,)), ((), ()))
    return lax.dot_general(left, right, dims, preferred_element_type=F32)


def three_pieces(value):
    high = value.astype(BF16).astype(F32)
    middle = (value - high).astype(BF16).astype(F32)
    return high, middle, value - high - middle


def occupied(sizes, chunk, _, colloc_hbm, coeffs_hbm, copies, block, sums, colloc, coeffs, sems):
    size_x, size_z, per_rows = sizes
    width, group = coeffs.shape
    points = colloc.shape[0]
    starts = range(0, width, chunk)
    copies_in = []
    for k, at in enumerate(starts):
        part = pl.ds(at, min(chunk, width - at))
        copies_in.append(
            (
                pltpu.make_async_copy(colloc_hbm.at[:, part], colloc.at[:, part], sems.at[0, k]),
                pltpu.make_async_copy(coeffs_hbm.at[part, :], coeffs.at[part, :], sems.at[1, k]),
            )
        )
    for first, second in copies_in:
        first.start()
        second.start()
    acc = jnp.zeros((points, group), F32)
    for (first, second), at in zip(copies_in, starts):
        first.wait()
        second.wait()
        part = pl.ds(at, min(chunk, width - at))
        acc += times(colloc[:, part], coeffs[part, :])
    occ = acc.astype(BF16)
    vals = occ.astype(F32)
    density = jnp.sum(vals * vals, axis=1, keepdims=True).astype(BF16)
    square = one_hot((points, points), lambda rows: rows)
    density = times(jnp.broadcast_to(density, (points, LANES)), square, 0, 0)[: sums.shape[1]]
    own = size_x * per_rows

    def source(col):
        return ((col % own) // per_rows) * (size_z * per_rows) + (col // own) * per_rows + col % per_rows

    pick = one_hot((LANES, LANES), lambda rows: jnp.where(rows < W, source(rows), -1))
    window = times(colloc[:, :LANES], pick, 1, 1)
    block[:, :group] = occ
    block[:, group:] = window.astype(BF16)
    for a in range(size_x):
        sums[a] = density
        copies[a] = occ


def potential_rows(sums, block, core, copies, density, shares):
    size_x, _, points = sums.shape
    size_y = copies.shape[0]
    group = block.shape[1] - LANES
    for a in range(size_x):
        density[:, a * points : (a + 1) * points] = sums[a]
    right = jnp.broadcast_to(density[:1, :], (LANES, size_x * points)).astype(BF16)
    lane = lax.broadcasted_iota(jnp.int32, (points, LANES), 1)
    occ = block[:, :group]
    window = block[:, group:].astype(F32)
    halves = core.shape[0] // (size_y * points)
    for half in range(halves):
        at = half * size_y * points
        shares[pl.ds(at, size_y * points), :] = times(core[pl.ds(at, size_y * points), :], right, 1, 1)
    for y in range(size_y):
        tail = window
        for half in range(halves):
            share = shares[pl.ds((half * size_y + y) * points, points), :]
            for k, piece in enumerate(three_pieces(share)):
                tail = jnp.where(lane == W + 3 * half + k, piece, tail)
        copies[y, :, :group] = occ
        copies[y, :, group:] = tail.astype(BF16)


def add_rows(per_step, rows, half, right, core, totals, tails):
    size_y, points, _ = rows.shape
    group = right.shape[1]
    height = per_step * points
    for y in range(0, size_y, per_step):
        left = rows[pl.ds(y, per_step), :, :group].reshape(height, group)
        tail = rows[pl.ds(y, per_step), :, group:].reshape(height, LANES)
        gram = times(left, right, 1, 1)
        at = pl.multiple_of(half * (size_y * points) + y * points, points)
        mixed = (core[pl.ds(at, height), :].astype(F32) * gram).astype(BF16)
        totals += times(tail, mixed, 0, 0)
        for step in range(per_step):
            tails += tail[step * points : (step + 1) * points].astype(F32)
    return totals, tails


def after(cols, mark):
    mark[...] = cols[0, :SUBLANES, :LANES].astype(F32)


def partial_totals(sizes, per_step, place, _, near, far, cols, core, sent, stored):
    size_x, size_z, per_rows = sizes
    points = far.shape[1]
    own = size_x * per_rows
    right = cols[...].reshape(-1, cols.shape[2])
    totals = jnp.zeros((LANES, right.shape[0]), F32)
    tails = jnp.zeros((points, LANES), F32)
    totals, tails = add_rows(per_step, near, place[2], right, core, totals, tails)
    totals, tails = add_rows(per_step, far, 1 - place[2], right, core, totals, tails)
    lane = lax.broadcasted_iota(jnp.int32, (points, LANES), 1)
    first = W + 3 * place[2]
    kept = (lane >= first) & (lane < first + 3)
    share = jnp.sum(jnp.where(kept, tails, 0.0), axis=1, keepdims=True)
    per_row = points // own
    point = lax.broadcasted_iota(jnp.int32, (points, LANES), 0)
    behind = W + 3 * (point % per_row)
    packed = jnp.zeros((points, LANES), F32)
    for k, piece in enumerate(three_pieces(share)):
        packed = jnp.where(lane == behind + k, piece, packed)
    fold_row = lax.broadcasted_iota(jnp.int32, (own, points), 0)
    fold_col = lax.broadcasted_iota(jnp.int32, (own, points), 1)
    fold = jnp.where(fold_col // per_row == fold_row, 1.0, 0.0).astype(BF16)
    packed = times(fold, packed.astype(BF16))
    stored[:, : size_x * points] = totals
    lane = lax.broadcasted_iota(jnp.int32, (LANES, LANES), 1)
    for a in range(size_x):
        start = a * points // LANES * LANES
        shift = a * points - start
        found = stored[:, pl.ds(start, 2 * LANES)]
        if shift:
            found = pltpu.roll(found, 2 * LANES - shift, 1)
        found = jnp.where(lane < points, found[:, :LANES], 0.0)
        carried = jnp.where(place[0] == a, packed, 0.0)
        for g in range(size_z):
            sent[a * size_z + g] = (found[g * own : (g + 1) * own] + carried).astype(BF16)


def final_shares(sizes, place, arrived, block, colloc, shares, rows):
    size_x, _, per_rows = sizes
    pieces, _, lanes = shares.shape
    wide = lanes // per_rows
    size_y = pieces // size_x
    part = colloc.shape[1] // size_y
    points = block.shape[0]
    own = size_x * per_rows
    per_row = points // own
    total = jnp.sum(arrived[...].astype(F32), axis=0)
    unfold_row = lax.broadcasted_iota(jnp.int32, (points, own), 0)
    unfold_col = lax.broadcasted_iota(jnp.int32, (points, own), 1)
    unfold = jnp.where(unfold_row // per_row == unfold_col, 1.0, 0.0).astype(BF16)
    spread_out = jnp.zeros((points, LANES), F32)
    for piece in three_pieces(total):
        spread_out += times(unfold, piece.astype(BF16))
    lane = lax.broadcasted_iota(jnp.int32, (points, LANES), 1)
    behind = W + 3 * (lax.broadcasted_iota(jnp.int32, (points, LANES), 0) % per_row)
    kept = (lane >= behind) & (lane < behind + 3)
    potential = jnp.sum(jnp.where(kept, spread_out, 0.0), axis=1, keepdims=True)
    window = block[:, block.shape[1] - LANES :]
    pick = one_hot((own, LANES), lambda row: row + place[1] * own)
    weighted = (times(window, pick, 1, 1) * potential).astype(BF16)

    def spread(which):
        def target(row):
            inside = row % SUBLANES
            found = (row // SUBLANES) * per_rows + inside // 2
            return jnp.where((inside % 2 == which) & (inside // 2 < per_rows), found, -1)

        return one_hot((size_x * SUBLANES, own), target)

    left = times(spread(0), weighted, 1, 1) + times(spread(1), total[:, :points].astype(BF16))
    rows[:, : colloc.shape[1]] = times(left.astype(BF16), colloc[...])
    for c in range(size_y):
        start = c * part // LANES * LANES
        span = wide + LANES
        found = rows[:, pl.ds(start, span)]
        shift = c * part - start
        if shift:
            found = pltpu.roll(found, span - shift, 1)
        found = found[:, :wide].astype(BF16)
        for a in range(size_x):
            for b in range(per_rows):
                at = a * SUBLANES + 2 * b
                shares[a * size_y + c, :, b * wide : (b + 1) * wide] = found[at : at + 2]


def outputs(arrived, coulomb, exchange):
    per_rows, part = coulomb.shape
    wide = arrived.shape[2] // per_rows
    total = jnp.sum(arrived[...].astype(F32), axis=0)
    for b in range(per_rows):
        at = b * wide
        coulomb[b : b + 1] = total[:1, at : at + part]
        exchange[b : b + 1] = total[1:, at : at + part]


def work(colloc, occ_coeffs, core):
    points, width = colloc.shape
    group = occ_coeffs.shape[1]
    size_x = lax.axis_size("gx")
    near_y = lax.axis_size("gy_1")
    size_y = lax.axis_size(GY)
    size_z = lax.axis_size("gz")
    row_count = core.shape[0]
    flat_cols = core.shape[2]
    per_rows = W // (size_x * size_z)
    own = size_x * per_rows
    part = width // size_y
    wide = -(-part // LANES) * LANES
    sizes = (size_x, size_z, per_rows)
    core_flat = core.reshape(row_count, flat_cols)
    place = jnp.stack([lax.axis_index("gx"), lax.axis_index("gz"), lax.axis_index("gy_0")])
    place = place.astype(jnp.int32)
    chunk = 8 * LANES
    steps = -(-width // chunk)

    copies, block, sums = pl.pallas_call(
        functools.partial(occupied, sizes, chunk),
        in_specs=[IN_SMEM, IN_HBM, IN_HBM],
        out_specs=[IN_VMEM, IN_VMEM, IN_VMEM],
        out_shape=[
            jax.ShapeDtypeStruct((size_x, points, group), BF16),
            jax.ShapeDtypeStruct((points, group + LANES), BF16),
            jax.ShapeDtypeStruct((size_x, 8, points), F32),
        ],
        scratch_shapes=[
            pltpu.VMEM((points, width), BF16),
            pltpu.VMEM((width, group), BF16),
            pltpu.SemaphoreType.DMA((2, steps)),
        ],
        compiler_params=pltpu.CompilerParams(vmem_limit_bytes=53 * 1024 * 1024),
        name="occupied",
    )(place, colloc, occ_coeffs)
    sums = exchange_pieces(sums, "gx")

    row_copies = pl.pallas_call(
        potential_rows,
        in_specs=[IN_VMEM, IN_VMEM, IN_VMEM],
        out_specs=IN_VMEM,
        out_shape=jax.ShapeDtypeStruct((near_y, points, group + LANES), BF16),
        scratch_shapes=[pltpu.VMEM((8, flat_cols), F32), pltpu.VMEM((row_count, LANES), F32)],
        compiler_params=PARAMS,
        name="potential_rows",
    )(sums, block, core_flat)
    near = exchange_pieces(row_copies, "gy_1")
    far = lax.ppermute(near, "gy_0", [(0, 1), (1, 0)])
    cols = exchange_pieces(copies, "gx")

    mark = pl.pallas_call(
        after,
        in_specs=[IN_VMEM],
        out_specs=IN_VMEM,
        out_shape=jax.ShapeDtypeStruct((SUBLANES, LANES), F32),
        compiler_params=PARAMS,
        name="after",
    )(cols)
    sent = pl.pallas_call(
        functools.partial(partial_totals, sizes, 4),
        in_specs=[IN_SMEM, IN_VMEM, IN_VMEM, IN_VMEM, IN_VMEM, IN_VMEM],
        out_specs=IN_VMEM,
        out_shape=jax.ShapeDtypeStruct((size_x * size_z, own, LANES), BF16),
        scratch_shapes=[pltpu.VMEM((LANES, flat_cols + LANES), F32)],
        compiler_params=PARAMS,
        name="partial_totals",
    )(place, mark, near, far, cols, core_flat)
    arrived = exchange_pieces(sent, ("gx", "gz"))

    shares = pl.pallas_call(
        functools.partial(final_shares, sizes),
        in_specs=[IN_SMEM, IN_VMEM, IN_VMEM, IN_VMEM],
        out_specs=IN_VMEM,
        out_shape=jax.ShapeDtypeStruct((size_x * size_y, 2, per_rows * wide), BF16),
        scratch_shapes=[pltpu.VMEM((size_x * SUBLANES, (width // LANES + 2) * LANES), F32)],
        compiler_params=PARAMS,
        name="final_shares",
    )(place, arrived, block, colloc)
    arrived = exchange_pieces(shares, GX_GY)
    return pl.pallas_call(
        outputs,
        in_specs=[IN_VMEM],
        out_specs=[IN_VMEM, IN_VMEM],
        out_shape=[jax.ShapeDtypeStruct((per_rows, part), F32)] * 2,
        compiler_params=PARAMS,
        name="outputs",
    )(arrived)


def solution(mesh):
    split = Mesh(
        mesh.devices.reshape(mesh.shape["gx"], 2, 8, mesh.shape["gz"]), ("gx", "gy_0", "gy_1", "gz")
    )
    return jax.shard_map(
        work,
        mesh=split,
        in_specs=(P(GX_GY, None), P(None, "gz"), P("gx", GY, None)),
        out_specs=(P(("gx", "gz"), GY), P(("gx", "gz"), GY)),
        check_vma=False,
    )
```

```python
import functools

import jax
import jax.numpy as jnp
from jax import lax
from jax.experimental import pallas as pl
from jax.experimental.pallas import tpu as pltpu
from jax.sharding import Mesh
from jax.sharding import PartitionSpec as P

W = 96
LANES = 128
SUBLANES = 8
GRANT = 24 * 1024 * 1024
GY = ("gy_0", "gy_1")
GX_GY = ("gx", "gy_0", "gy_1")
BF16 = jnp.bfloat16
F32 = jnp.float32
IN_VMEM = pl.BlockSpec(memory_space=pltpu.VMEM)
IN_HBM = pl.BlockSpec(memory_space=pltpu.HBM)
IN_SMEM = pl.BlockSpec(memory_space=pltpu.SMEM)
PARAMS = pltpu.CompilerParams(vmem_limit_bytes=GRANT)


def exchange_pieces(pieces, axis):
    return lax.all_to_all(pieces, axis, split_axis=0, concat_axis=0, tiled=True)


def one_hot(shape, target):
    rows = lax.broadcasted_iota(jnp.int32, shape, 0)
    cols = lax.broadcasted_iota(jnp.int32, shape, 1)
    return jnp.where(cols == target(rows), 1.0, 0.0).astype(BF16)


def times(left, right, left_dim=1, right_dim=0):
    dims = (((left_dim,), (right_dim,)), ((), ()))
    return lax.dot_general(left, right, dims, preferred_element_type=F32)


PIECES = 2


def in_pieces(value):
    high = value.astype(BF16).astype(F32)
    return high, value - high


def occupied(sizes, chunk, _, colloc_hbm, coeffs_hbm, copies, block, sums, colloc, coeffs, sems):
    size_x, size_z, per_rows = sizes
    width, group = coeffs.shape
    points = colloc.shape[0]
    starts = range(0, width, chunk)
    copies_in = []
    for k, at in enumerate(starts):
        part = pl.ds(at, min(chunk, width - at))
        copies_in.append(
            (
                pltpu.make_async_copy(colloc_hbm.at[:, part], colloc.at[:, part], sems.at[0, k]),
                pltpu.make_async_copy(coeffs_hbm.at[part, :], coeffs.at[part, :], sems.at[1, k]),
            )
        )
    for first, second in copies_in:
        first.start()
        second.start()
    own = size_x * per_rows

    def source(col):
        return ((col % own) // per_rows) * (size_z * per_rows) + (col // own) * per_rows + col % per_rows

    pick = one_hot((LANES, LANES), lambda rows: jnp.where(rows < W, source(rows), -1))
    square = one_hot((points, points), lambda rows: rows)
    acc = jnp.zeros((points, group), F32)
    for (first, second), at in zip(copies_in, starts):
        first.wait()
        second.wait()
        part = pl.ds(at, min(chunk, width - at))
        acc += times(colloc[:, part], coeffs[part, :])
        if at == 0:
            block[:, group:] = times(colloc[:, :LANES], pick, 1, 1).astype(BF16)
    occ = acc.astype(BF16)
    vals = occ.astype(F32)
    density = jnp.sum(vals * vals, axis=1, keepdims=True).astype(BF16)
    density = times(jnp.broadcast_to(density, (points, LANES)), square, 0, 0)[: sums.shape[1]]
    block[:, :group] = occ
    for a in range(size_x):
        sums[a] = density
        copies[a] = occ


def potential_rows(sums, block, core, copies, density, shares):
    size_x, _, points = sums.shape
    size_y = copies.shape[0]
    group = block.shape[1] - LANES
    for a in range(size_x):
        density[:, a * points : (a + 1) * points] = sums[a]
    right = jnp.broadcast_to(density[:1, :], (LANES, size_x * points)).astype(BF16)
    lane = lax.broadcasted_iota(jnp.int32, (points, LANES), 1)
    occ = block[:, :group]
    window = block[:, group:].astype(F32)
    halves = core.shape[0] // (size_y * points)
    for half in range(halves):
        at = half * size_y * points
        shares[pl.ds(at, size_y * points), :] = times(core[pl.ds(at, size_y * points), :], right, 1, 1)
    for y in range(size_y):
        tail = window
        for half in range(halves):
            share = shares[pl.ds((half * size_y + y) * points, points), :]
            for k, piece in enumerate(in_pieces(share)):
                tail = jnp.where(lane == W + PIECES * half + k, piece, tail)
        copies[y, :, :group] = occ
        copies[y, :, group:] = tail.astype(BF16)


def add_rows(per_step, rows, half, right, core, totals, tails):
    size_y, points, _ = rows.shape
    group = right.shape[1]
    height = per_step * points
    for y in range(0, size_y, per_step):
        left = rows[pl.ds(y, per_step), :, :group].reshape(height, group)
        tail = rows[pl.ds(y, per_step), :, group:].reshape(height, LANES)
        gram = times(left, right, 1, 1)
        at = pl.multiple_of(half * (size_y * points) + y * points, points)
        mixed = (core[pl.ds(at, height), :].astype(F32) * gram).astype(BF16)
        totals += times(tail, mixed, 0, 0)
        for step in range(per_step):
            tails += tail[step * points : (step + 1) * points].astype(F32)
    return totals, tails


def after(cols, mark):
    mark[...] = cols[0, :SUBLANES, :LANES].astype(F32)


def partial_totals(sizes, per_step, place, _, near, far, cols, core, sent, stored):
    size_x, size_z, per_rows = sizes
    points = far.shape[1]
    own = size_x * per_rows
    right = cols[...].reshape(-1, cols.shape[2])
    totals = jnp.zeros((LANES, right.shape[0]), F32)
    tails = jnp.zeros((points, LANES), F32)
    totals, tails = add_rows(per_step, near, place[2], right, core, totals, tails)
    totals, tails = add_rows(per_step, far, 1 - place[2], right, core, totals, tails)
    lane = lax.broadcasted_iota(jnp.int32, (points, LANES), 1)
    first = W + PIECES * place[2]
    kept = (lane >= first) & (lane < first + PIECES)
    share = jnp.sum(jnp.where(kept, tails, 0.0), axis=1, keepdims=True)
    per_row = points // own
    point = lax.broadcasted_iota(jnp.int32, (points, LANES), 0)
    behind = W + PIECES * (point % per_row)
    packed = jnp.zeros((points, LANES), F32)
    for k, piece in enumerate(in_pieces(share)):
        packed = jnp.where(lane == behind + k, piece, packed)
    fold_row = lax.broadcasted_iota(jnp.int32, (own, points), 0)
    fold_col = lax.broadcasted_iota(jnp.int32, (own, points), 1)
    fold = jnp.where(fold_col // per_row == fold_row, 1.0, 0.0).astype(BF16)
    packed = times(fold, packed.astype(BF16))
    stored[:, : size_x * points] = totals
    lane = lax.broadcasted_iota(jnp.int32, (LANES, LANES), 1)
    for a in range(size_x):
        start = a * points // LANES * LANES
        shift = a * points - start
        found = stored[:, pl.ds(start, 2 * LANES)]
        if shift:
            found = pltpu.roll(found, 2 * LANES - shift, 1)
        found = jnp.where(lane < points, found[:, :LANES], 0.0)
        carried = jnp.where(place[0] == a, packed, 0.0)
        for g in range(size_z):
            sent[a * size_z + g] = (found[g * own : (g + 1) * own] + carried).astype(BF16)


def final_shares(sizes, place, arrived, block, colloc, shares, rows):
    size_x, _, per_rows = sizes
    pieces, height, lanes = shares.shape
    wide = height * lanes // (2 * per_rows)
    size_y = pieces // size_x
    part = colloc.shape[1] // size_y
    points = block.shape[0]
    own = size_x * per_rows
    per_row = points // own
    total = jnp.sum(arrived[...].astype(F32), axis=0)
    unfold_row = lax.broadcasted_iota(jnp.int32, (points, own), 0)
    unfold_col = lax.broadcasted_iota(jnp.int32, (points, own), 1)
    unfold = jnp.where(unfold_row // per_row == unfold_col, 1.0, 0.0).astype(BF16)
    spread_out = jnp.zeros((points, LANES), F32)
    for piece in in_pieces(total):
        spread_out += times(unfold, piece.astype(BF16))
    lane = lax.broadcasted_iota(jnp.int32, (points, LANES), 1)
    behind = W + PIECES * (lax.broadcasted_iota(jnp.int32, (points, LANES), 0) % per_row)
    kept = (lane >= behind) & (lane < behind + PIECES)
    potential = jnp.sum(jnp.where(kept, spread_out, 0.0), axis=1, keepdims=True)
    window = block[:, block.shape[1] - LANES :]
    pick = one_hot((own, LANES), lambda row: row + place[1] * own)
    weighted = (times(window, pick, 1, 1) * potential).astype(BF16)

    def spread(which):
        def target(row):
            inside = row % SUBLANES
            found = (row // SUBLANES) * per_rows + inside // 2
            return jnp.where((inside % 2 == which) & (inside // 2 < per_rows), found, -1)

        return one_hot((size_x * SUBLANES, own), target)

    left = times(spread(0), weighted, 1, 1) + times(spread(1), total[:, :points].astype(BF16))
    left = left.astype(BF16)
    width = colloc.shape[1]
    step = 4 * LANES
    for at in range(0, width, step):
        part_of = pl.ds(at, min(step, width - at))
        rows[:, part_of] = times(left, colloc[:, part_of])
    for c in range(size_y):
        start = c * part // LANES * LANES
        span = wide + LANES
        found = rows[:, pl.ds(start, span)]
        shift = c * part - start
        if shift:
            found = pltpu.roll(found, span - shift, 1)
        found = found[:, :wide].astype(BF16)
        for a in range(size_x):
            for b in range(per_rows):
                at = a * SUBLANES + 2 * b
                for lanes in range(0, wide, LANES):
                    row, place_in = divmod(b * wide + lanes, shares.shape[2])
                    shares[a * size_y + c, 2 * row : 2 * row + 2, place_in : place_in + LANES] = found[
                        at : at + 2, lanes : lanes + LANES
                    ]


def outputs(arrived, coulomb, exchange):
    per_rows, part = coulomb.shape
    _, height, lanes = arrived.shape
    wide = height * lanes // (2 * per_rows)
    total = jnp.sum(arrived[...].astype(F32), axis=0)
    joined = jnp.concatenate([total[row : row + 2] for row in range(0, height, 2)], axis=1)
    for b in range(per_rows):
        at = b * wide
        coulomb[b : b + 1] = joined[:1, at : at + part]
        exchange[b : b + 1] = joined[1:, at : at + part]


def work(colloc, occ_coeffs, core):
    points, width = colloc.shape
    group = occ_coeffs.shape[1]
    size_x = lax.axis_size("gx")
    near_y = lax.axis_size("gy_1")
    size_y = lax.axis_size(GY)
    size_z = lax.axis_size("gz")
    row_count = core.shape[0]
    flat_cols = core.shape[2]
    per_rows = W // (size_x * size_z)
    own = size_x * per_rows
    part = width // size_y
    wide = -(-part // LANES) * LANES
    sizes = (size_x, size_z, per_rows)
    core_flat = core.reshape(row_count, flat_cols)
    place = jnp.stack([lax.axis_index("gx"), lax.axis_index("gz"), lax.axis_index("gy_0")])
    place = place.astype(jnp.int32)
    chunk = 8 * LANES
    steps = -(-width // chunk)

    copies, block, sums = pl.pallas_call(
        functools.partial(occupied, sizes, chunk),
        in_specs=[IN_SMEM, IN_HBM, IN_HBM],
        out_specs=[IN_VMEM, IN_VMEM, IN_VMEM],
        out_shape=[
            jax.ShapeDtypeStruct((size_x, points, group), BF16),
            jax.ShapeDtypeStruct((points, group + LANES), BF16),
            jax.ShapeDtypeStruct((size_x, 8, points), F32),
        ],
        scratch_shapes=[
            pltpu.VMEM((points, width), BF16),
            pltpu.VMEM((width, group), BF16),
            pltpu.SemaphoreType.DMA((2, steps)),
        ],
        compiler_params=pltpu.CompilerParams(vmem_limit_bytes=53 * 1024 * 1024),
        name="occupied",
    )(place, colloc, occ_coeffs)
    sums = exchange_pieces(sums, "gx")

    row_copies = pl.pallas_call(
        potential_rows,
        in_specs=[IN_VMEM, IN_VMEM, IN_VMEM],
        out_specs=IN_VMEM,
        out_shape=jax.ShapeDtypeStruct((near_y, points, group + LANES), BF16),
        scratch_shapes=[pltpu.VMEM((8, flat_cols), F32), pltpu.VMEM((row_count, LANES), F32)],
        compiler_params=PARAMS,
        name="potential_rows",
    )(sums, block, core_flat)
    near = exchange_pieces(row_copies, "gy_1")
    far = lax.ppermute(near, "gy_0", [(0, 1), (1, 0)])
    cols = exchange_pieces(copies, "gx")

    mark = pl.pallas_call(
        after,
        in_specs=[IN_VMEM],
        out_specs=IN_VMEM,
        out_shape=jax.ShapeDtypeStruct((SUBLANES, LANES), F32),
        compiler_params=PARAMS,
        name="after",
    )(cols)
    sent = pl.pallas_call(
        functools.partial(partial_totals, sizes, 8),
        in_specs=[IN_SMEM, IN_VMEM, IN_VMEM, IN_VMEM, IN_VMEM, IN_VMEM],
        out_specs=IN_VMEM,
        out_shape=jax.ShapeDtypeStruct((size_x * size_z, own, LANES), BF16),
        scratch_shapes=[pltpu.VMEM((LANES, flat_cols + LANES), F32)],
        compiler_params=PARAMS,
        name="partial_totals",
    )(place, mark, near, far, cols, core_flat)
    arrived = exchange_pieces(sent, ("gx", "gz"))

    shares = pl.pallas_call(
        functools.partial(final_shares, sizes),
        in_specs=[IN_SMEM, IN_VMEM, IN_VMEM, IN_VMEM],
        out_specs=IN_VMEM,
        out_shape=jax.ShapeDtypeStruct((size_x * size_y, 4, per_rows * wide // 2), BF16),
        scratch_shapes=[pltpu.VMEM((size_x * SUBLANES, (width // LANES + 2) * LANES), F32)],
        compiler_params=PARAMS,
        name="final_shares",
    )(place, arrived, block, colloc)
    arrived = exchange_pieces(shares, GX_GY)
    return pl.pallas_call(
        outputs,
        in_specs=[IN_VMEM],
        out_specs=[IN_VMEM, IN_VMEM],
        out_shape=[jax.ShapeDtypeStruct((per_rows, part), F32)] * 2,
        compiler_params=PARAMS,
        name="outputs",
    )(arrived)


def solution(mesh):
    split = Mesh(
        mesh.devices.reshape(mesh.shape["gx"], 2, 8, mesh.shape["gz"]), ("gx", "gy_0", "gy_1", "gz")
    )
    return jax.shard_map(
        work,
        mesh=split,
        in_specs=(P(GX_GY, None), P(None, "gz"), P("gx", GY, None)),
        out_specs=(P(("gx", "gz"), GY), P(("gx", "gz"), GY)),
        check_vma=False,
    )
```

```python
import functools

import jax
import jax.numpy as jnp
from jax import lax
from jax.experimental import pallas as pl
from jax.experimental.pallas import tpu as pltpu
from jax.sharding import Mesh
from jax.sharding import PartitionSpec as P

W = 96
LANES = 128
SUBLANES = 8
GRANT = 24 * 1024 * 1024
GY = ("gy_0", "gy_1")
GX_GY = ("gx", "gy_0", "gy_1")
BF16 = jnp.bfloat16
F32 = jnp.float32
IN_VMEM = pl.BlockSpec(memory_space=pltpu.VMEM)
IN_HBM = pl.BlockSpec(memory_space=pltpu.HBM)
IN_SMEM = pl.BlockSpec(memory_space=pltpu.SMEM)
PARAMS = pltpu.CompilerParams(vmem_limit_bytes=GRANT)


def exchange_pieces(pieces, axis):
    return lax.all_to_all(pieces, axis, split_axis=0, concat_axis=0, tiled=True)


def one_hot(shape, target):
    rows = lax.broadcasted_iota(jnp.int32, shape, 0)
    cols = lax.broadcasted_iota(jnp.int32, shape, 1)
    return jnp.where(cols == target(rows), 1.0, 0.0).astype(BF16)


def times(left, right, left_dim=1, right_dim=0):
    dims = (((left_dim,), (right_dim,)), ((), ()))
    return lax.dot_general(left, right, dims, preferred_element_type=F32)


PIECES = 2


def in_pieces(value):
    high = value.astype(BF16).astype(F32)
    return high, value - high


def occupied(sizes, chunk, _, colloc_hbm, coeffs_hbm, copies, block, sums, colloc, coeffs, sems):
    size_x, size_z, per_rows = sizes
    width, group = coeffs.shape
    points = colloc.shape[0]
    starts = range(0, width, chunk)
    copies_in = []
    for k, at in enumerate(starts):
        part = pl.ds(at, min(chunk, width - at))
        copies_in.append(
            (
                pltpu.make_async_copy(colloc_hbm.at[:, part], colloc.at[:, part], sems.at[0, k]),
                pltpu.make_async_copy(coeffs_hbm.at[part, :], coeffs.at[part, :], sems.at[1, k]),
            )
        )
    for first, second in copies_in:
        first.start()
        second.start()
    own = size_x * per_rows

    def source(col):
        return ((col % own) // per_rows) * (size_z * per_rows) + (col // own) * per_rows + col % per_rows

    pick = one_hot((LANES, LANES), lambda rows: jnp.where(rows < W, source(rows), -1))
    square = one_hot((points, LANES), lambda rows: rows)
    acc = jnp.zeros((points, group), F32)
    for (first, second), at in zip(copies_in, starts):
        first.wait()
        second.wait()
        part = pl.ds(at, min(chunk, width - at))
        acc += times(colloc[:, part], coeffs[part, :])
        if at == 0:
            block[:, group:] = times(colloc[:, :LANES], pick, 1, 1).astype(BF16)
    occ = acc.astype(BF16)
    vals = occ.astype(F32)
    density = jnp.sum(vals * vals, axis=1, keepdims=True).astype(BF16)
    density = times(jnp.broadcast_to(density, (points, LANES)), square, 0, 0)[: sums.shape[1]].astype(BF16)
    block[:, :group] = occ
    for a in range(size_x):
        sums[a] = density
        copies[a] = occ


def potential_rows(sums, block, core, copies, density, shares):
    size_x = sums.shape[0]
    size_y, points, _ = copies.shape
    group = block.shape[1] - LANES
    for a in range(size_x):
        density[:2, a * points : (a + 1) * points] = sums[a].astype(F32)[:, :points]
    right = jnp.broadcast_to(density[:1, :], (LANES, size_x * points)).astype(BF16)
    lane = lax.broadcasted_iota(jnp.int32, (points, LANES), 1)
    occ = block[:, :group]
    window = block[:, group:].astype(F32)
    halves = core.shape[0] // (size_y * points)
    for half in range(halves):
        at = half * size_y * points
        shares[pl.ds(at, size_y * points), :] = times(core[pl.ds(at, size_y * points), :], right, 1, 1)
    for y in range(size_y):
        tail = window
        for half in range(halves):
            share = shares[pl.ds((half * size_y + y) * points, points), :]
            for k, piece in enumerate(in_pieces(share)):
                tail = jnp.where(lane == W + PIECES * half + k, piece, tail)
        copies[y, :, :group] = occ
        copies[y, :, group:] = tail.astype(BF16)


def add_rows(per_step, rows, half, right, core, totals, tails):
    size_y, points, _ = rows.shape
    group = right.shape[1]
    height = per_step * points
    for y in range(0, size_y, per_step):
        left = rows[pl.ds(y, per_step), :, :group].reshape(height, group)
        tail = rows[pl.ds(y, per_step), :, group:].reshape(height, LANES)
        gram = times(left, right, 1, 1)
        at = pl.multiple_of(half * (size_y * points) + y * points, points)
        mixed = (core[pl.ds(at, height), :].astype(F32) * gram).astype(BF16)
        totals += times(tail, mixed, 0, 0)
        for step in range(per_step):
            tails += tail[step * points : (step + 1) * points].astype(F32)
    return totals, tails


def after(cols, mark):
    mark[...] = cols[0, :SUBLANES, :LANES].astype(F32)


def partial_totals(sizes, per_step, place, _, near, far, cols, core, sent, stored):
    size_x, size_z, per_rows = sizes
    points = far.shape[1]
    own = size_x * per_rows
    right = cols[...].reshape(-1, cols.shape[2])
    totals = jnp.zeros((LANES, right.shape[0]), F32)
    tails = jnp.zeros((points, LANES), F32)
    totals, tails = add_rows(per_step, near, place[2], right, core, totals, tails)
    totals, tails = add_rows(per_step, far, 1 - place[2], right, core, totals, tails)
    lane = lax.broadcasted_iota(jnp.int32, (points, LANES), 1)
    first = W + PIECES * place[2]
    kept = (lane >= first) & (lane < first + PIECES)
    share = jnp.sum(jnp.where(kept, tails, 0.0), axis=1, keepdims=True)
    per_row = points // own
    point = lax.broadcasted_iota(jnp.int32, (points, LANES), 0)
    behind = W + PIECES * (point % per_row)
    packed = jnp.zeros((points, LANES), F32)
    for k, piece in enumerate(in_pieces(share)):
        packed = jnp.where(lane == behind + k, piece, packed)
    fold_row = lax.broadcasted_iota(jnp.int32, (own, points), 0)
    fold_col = lax.broadcasted_iota(jnp.int32, (own, points), 1)
    fold = jnp.where(fold_col // per_row == fold_row, 1.0, 0.0).astype(BF16)
    packed = times(fold, packed.astype(BF16))
    stored[:, : size_x * points] = totals
    lane = lax.broadcasted_iota(jnp.int32, (LANES, LANES), 1)
    for a in range(size_x):
        start = a * points // LANES * LANES
        shift = a * points - start
        found = stored[:, pl.ds(start, 2 * LANES)]
        if shift:
            found = pltpu.roll(found, 2 * LANES - shift, 1)
        found = jnp.where(lane < points, found[:, :LANES], 0.0)
        carried = jnp.where(place[0] == a, packed, 0.0)
        for g in range(size_z):
            sent[a * size_z + g] = (found[g * own : (g + 1) * own] + carried).astype(BF16)


def final_shares(sizes, place, arrived, block, colloc, shares, rows):
    size_x, _, per_rows = sizes
    pieces, height, lanes = shares.shape
    wide = height * lanes // (2 * per_rows)
    size_y = pieces // size_x
    part = colloc.shape[1] // size_y
    points = block.shape[0]
    own = size_x * per_rows
    per_row = points // own
    total = jnp.sum(arrived[...].astype(F32), axis=0)
    unfold_row = lax.broadcasted_iota(jnp.int32, (points, own), 0)
    unfold_col = lax.broadcasted_iota(jnp.int32, (points, own), 1)
    unfold = jnp.where(unfold_row // per_row == unfold_col, 1.0, 0.0).astype(BF16)
    spread_out = jnp.zeros((points, LANES), F32)
    for piece in in_pieces(total):
        spread_out += times(unfold, piece.astype(BF16))
    lane = lax.broadcasted_iota(jnp.int32, (points, LANES), 1)
    behind = W + PIECES * (lax.broadcasted_iota(jnp.int32, (points, LANES), 0) % per_row)
    kept = (lane >= behind) & (lane < behind + PIECES)
    potential = jnp.sum(jnp.where(kept, spread_out, 0.0), axis=1, keepdims=True)
    window = block[:, block.shape[1] - LANES :]
    pick = one_hot((own, LANES), lambda row: row + place[1] * own)
    weighted = (times(window, pick, 1, 1) * potential).astype(BF16)

    def spread(which):
        def target(row):
            inside = row % SUBLANES
            found = (row // SUBLANES) * per_rows + inside // 2
            return jnp.where((inside % 2 == which) & (inside // 2 < per_rows), found, -1)

        return one_hot((size_x * SUBLANES, own), target)

    left = times(spread(0), weighted, 1, 1) + times(spread(1), total[:, :points].astype(BF16))
    left = left.astype(BF16)
    width = colloc.shape[1]
    step = 4 * LANES
    for at in range(0, width, step):
        part_of = pl.ds(at, min(step, width - at))
        rows[:, part_of] = times(left, colloc[:, part_of])
    for c in range(size_y):
        start = c * part // LANES * LANES
        span = wide + LANES
        found = rows[:, pl.ds(start, span)]
        shift = c * part - start
        if shift:
            found = pltpu.roll(found, span - shift, 1)
        found = found[:, :wide].astype(BF16)
        for a in range(size_x):
            for b in range(per_rows):
                at = a * SUBLANES + 2 * b
                for lanes in range(0, wide, LANES):
                    row, place_in = divmod(b * wide + lanes, shares.shape[2])
                    shares[a * size_y + c, 2 * row : 2 * row + 2, place_in : place_in + LANES] = found[
                        at : at + 2, lanes : lanes + LANES
                    ]


def outputs(arrived, coulomb, exchange):
    per_rows, part = coulomb.shape
    _, height, lanes = arrived.shape
    wide = height * lanes // (2 * per_rows)
    total = jnp.sum(arrived[...].astype(F32), axis=0)
    joined = jnp.concatenate([total[row : row + 2] for row in range(0, height, 2)], axis=1)
    for b in range(per_rows):
        at = b * wide
        coulomb[b : b + 1] = joined[:1, at : at + part]
        exchange[b : b + 1] = joined[1:, at : at + part]


def work(colloc, occ_coeffs, core):
    points, width = colloc.shape
    group = occ_coeffs.shape[1]
    size_x = lax.axis_size("gx")
    near_y = lax.axis_size("gy_1")
    size_y = lax.axis_size(GY)
    size_z = lax.axis_size("gz")
    row_count = core.shape[0]
    flat_cols = core.shape[2]
    per_rows = W // (size_x * size_z)
    own = size_x * per_rows
    part = width // size_y
    wide = -(-part // LANES) * LANES
    sizes = (size_x, size_z, per_rows)
    core_flat = core.reshape(row_count, flat_cols)
    place = jnp.stack([lax.axis_index("gx"), lax.axis_index("gz"), lax.axis_index("gy_0")])
    place = place.astype(jnp.int32)
    chunk = 8 * LANES
    steps = -(-width // chunk)

    copies, block, sums = pl.pallas_call(
        functools.partial(occupied, sizes, chunk),
        in_specs=[IN_SMEM, IN_HBM, IN_HBM],
        out_specs=[IN_VMEM, IN_VMEM, IN_VMEM],
        out_shape=[
            jax.ShapeDtypeStruct((size_x, points, group), BF16),
            jax.ShapeDtypeStruct((points, group + LANES), BF16),
            jax.ShapeDtypeStruct((size_x, 2, LANES), BF16),
        ],
        scratch_shapes=[
            pltpu.VMEM((points, width), BF16),
            pltpu.VMEM((width, group), BF16),
            pltpu.SemaphoreType.DMA((2, steps)),
        ],
        compiler_params=pltpu.CompilerParams(vmem_limit_bytes=53 * 1024 * 1024),
        name="occupied",
    )(place, colloc, occ_coeffs)
    sums = exchange_pieces(sums, "gx")

    row_copies = pl.pallas_call(
        potential_rows,
        in_specs=[IN_VMEM, IN_VMEM, IN_VMEM],
        out_specs=IN_VMEM,
        out_shape=jax.ShapeDtypeStruct((near_y, points, group + LANES), BF16),
        scratch_shapes=[pltpu.VMEM((8, flat_cols), F32), pltpu.VMEM((row_count, LANES), F32)],
        compiler_params=PARAMS,
        name="potential_rows",
    )(sums, block, core_flat)
    near = exchange_pieces(row_copies, "gy_1")
    far = lax.ppermute(near, "gy_0", [(0, 1), (1, 0)])
    cols = exchange_pieces(copies, "gx")

    mark = pl.pallas_call(
        after,
        in_specs=[IN_VMEM],
        out_specs=IN_VMEM,
        out_shape=jax.ShapeDtypeStruct((SUBLANES, LANES), F32),
        compiler_params=PARAMS,
        name="after",
    )(cols)
    sent = pl.pallas_call(
        functools.partial(partial_totals, sizes, 8),
        in_specs=[IN_SMEM, IN_VMEM, IN_VMEM, IN_VMEM, IN_VMEM, IN_VMEM],
        out_specs=IN_VMEM,
        out_shape=jax.ShapeDtypeStruct((size_x * size_z, own, LANES), BF16),
        scratch_shapes=[pltpu.VMEM((LANES, flat_cols + LANES), F32)],
        compiler_params=PARAMS,
        name="partial_totals",
    )(place, mark, near, far, cols, core_flat)
    arrived = exchange_pieces(sent, ("gx", "gz"))

    shares = pl.pallas_call(
        functools.partial(final_shares, sizes),
        in_specs=[IN_SMEM, IN_VMEM, IN_VMEM, IN_VMEM],
        out_specs=IN_VMEM,
        out_shape=jax.ShapeDtypeStruct((size_x * size_y, 4, per_rows * wide // 2), BF16),
        scratch_shapes=[pltpu.VMEM((size_x * SUBLANES, (width // LANES + 2) * LANES), F32)],
        compiler_params=PARAMS,
        name="final_shares",
    )(place, arrived, block, colloc)
    arrived = exchange_pieces(shares, GX_GY)
    return pl.pallas_call(
        outputs,
        in_specs=[IN_VMEM],
        out_specs=[IN_VMEM, IN_VMEM],
        out_shape=[jax.ShapeDtypeStruct((per_rows, part), F32)] * 2,
        compiler_params=PARAMS,
        name="outputs",
    )(arrived)


def solution(mesh):
    split = Mesh(
        mesh.devices.reshape(mesh.shape["gx"], 2, 8, mesh.shape["gz"]), ("gx", "gy_0", "gy_1", "gz")
    )
    return jax.shard_map(
        work,
        mesh=split,
        in_specs=(P(GX_GY, None), P(None, "gz"), P("gx", GY, None)),
        out_specs=(P(("gx", "gz"), GY), P(("gx", "gz"), GY)),
        check_vma=False,
    )
```

```python
import functools

import jax
import jax.numpy as jnp
from jax import lax
from jax.experimental import pallas as pl
from jax.experimental.pallas import tpu as pltpu
from jax.sharding import Mesh
from jax.sharding import PartitionSpec as P

W = 96
LANES = 128
SUBLANES = 8
GRANT = 24 * 1024 * 1024
GY = ("gy_0", "gy_1")
GX_GY = ("gx", "gy_0", "gy_1")
BF16 = jnp.bfloat16
F32 = jnp.float32
IN_VMEM = pl.BlockSpec(memory_space=pltpu.VMEM)
IN_HBM = pl.BlockSpec(memory_space=pltpu.HBM)
IN_SMEM = pl.BlockSpec(memory_space=pltpu.SMEM)
PARAMS = pltpu.CompilerParams(vmem_limit_bytes=GRANT)


def exchange_pieces(pieces, axis):
    return lax.all_to_all(pieces, axis, split_axis=0, concat_axis=0, tiled=True)


def one_hot(shape, target):
    rows = lax.broadcasted_iota(jnp.int32, shape, 0)
    cols = lax.broadcasted_iota(jnp.int32, shape, 1)
    return jnp.where(cols == target(rows), 1.0, 0.0).astype(BF16)


def times(left, right, left_dim=1, right_dim=0):
    dims = (((left_dim,), (right_dim,)), ((), ()))
    return lax.dot_general(left, right, dims, preferred_element_type=F32)


PIECES = 2


def in_pieces(value):
    high = value.astype(BF16).astype(F32)
    return high, value - high


def occupied(sizes, chunk, _, colloc_hbm, coeffs_hbm, copies, block, sums, colloc, coeffs, sems):
    size_x, size_z, per_rows = sizes
    width, group = coeffs.shape
    points = colloc.shape[0]
    starts = [0, chunk, 2 * chunk, width // LANES * LANES - 3 * LANES]
    widths = [after_it - at for at, after_it in zip(starts, starts[1:] + [width])]
    copies_in = []
    for k, (at, size) in enumerate(zip(starts, widths)):
        part = pl.ds(at, size)
        copies_in.append(
            (
                pltpu.make_async_copy(colloc_hbm.at[:, part], colloc.at[:, part], sems.at[0, k]),
                pltpu.make_async_copy(coeffs_hbm.at[part, :], coeffs.at[part, :], sems.at[1, k]),
            )
        )
    for first, second in copies_in:
        first.start()
        second.start()
    own = size_x * per_rows

    def source(col):
        return ((col % own) // per_rows) * (size_z * per_rows) + (col // own) * per_rows + col % per_rows

    pick = one_hot((LANES, LANES), lambda rows: jnp.where(rows < W, source(rows), -1))
    square = one_hot((points, LANES), lambda rows: rows)
    acc = jnp.zeros((points, group), F32)
    for (first, second), at, size in zip(copies_in, starts, widths):
        first.wait()
        second.wait()
        part = pl.ds(at, size)
        acc += times(colloc[:, part], coeffs[part, :])
        if at == 0:
            block[:, group:] = times(colloc[:, :LANES], pick, 1, 1).astype(BF16)
    occ = acc.astype(BF16)
    vals = occ.astype(F32)
    density = jnp.sum(vals * vals, axis=1, keepdims=True).astype(BF16)
    density = times(jnp.broadcast_to(density, (points, LANES)), square, 0, 0)[: sums.shape[1]].astype(BF16)
    block[:, :group] = occ
    for a in range(size_x):
        sums[a] = density
        copies[a] = occ


def potential_rows(sums, block, core, copies, density, shares):
    size_x = sums.shape[0]
    size_y, points, _ = copies.shape
    group = block.shape[1] - LANES
    for a in range(size_x):
        density[:2, a * points : (a + 1) * points] = sums[a].astype(F32)[:, :points]
    right = jnp.broadcast_to(density[:1, :], (LANES, size_x * points)).astype(BF16)
    lane = lax.broadcasted_iota(jnp.int32, (points, LANES), 1)
    occ = block[:, :group]
    window = block[:, group:].astype(F32)
    halves = core.shape[0] // (size_y * points)
    for half in range(halves):
        at = half * size_y * points
        shares[pl.ds(at, size_y * points), :] = times(core[pl.ds(at, size_y * points), :], right, 1, 1)
    for y in range(size_y):
        tail = window
        for half in range(halves):
            share = shares[pl.ds((half * size_y + y) * points, points), :]
            for k, piece in enumerate(in_pieces(share)):
                tail = jnp.where(lane == W + PIECES * half + k, piece, tail)
        copies[y, :, :group] = occ
        copies[y, :, group:] = tail.astype(BF16)


def add_rows(per_step, rows, half, right, core, totals, tails):
    size_y, points, _ = rows.shape
    group = right.shape[1]
    height = per_step * points
    for y in range(0, size_y, per_step):
        left = rows[pl.ds(y, per_step), :, :group].reshape(height, group)
        tail = rows[pl.ds(y, per_step), :, group:].reshape(height, LANES)
        gram = times(left, right, 1, 1)
        at = pl.multiple_of(half * (size_y * points) + y * points, points)
        mixed = (core[pl.ds(at, height), :].astype(F32) * gram).astype(BF16)
        totals += times(tail, mixed, 0, 0)
        for step in range(per_step):
            tails += tail[step * points : (step + 1) * points].astype(F32)
    return totals, tails


def after(cols, mark):
    mark[...] = cols[0, :SUBLANES, :LANES].astype(F32)


def partial_totals(sizes, per_step, place, _, near, far, cols, core, sent, stored):
    size_x, size_z, per_rows = sizes
    points = far.shape[1]
    own = size_x * per_rows
    right = cols[...].reshape(-1, cols.shape[2])
    totals = jnp.zeros((LANES, right.shape[0]), F32)
    tails = jnp.zeros((points, LANES), F32)
    totals, tails = add_rows(per_step, near, place[2], right, core, totals, tails)
    totals, tails = add_rows(per_step, far, 1 - place[2], right, core, totals, tails)
    lane = lax.broadcasted_iota(jnp.int32, (points, LANES), 1)
    first = W + PIECES * place[2]
    kept = (lane >= first) & (lane < first + PIECES)
    share = jnp.sum(jnp.where(kept, tails, 0.0), axis=1, keepdims=True)
    per_row = points // own
    point = lax.broadcasted_iota(jnp.int32, (points, LANES), 0)
    behind = W + PIECES * (point % per_row)
    packed = jnp.zeros((points, LANES), F32)
    for k, piece in enumerate(in_pieces(share)):
        packed = jnp.where(lane == behind + k, piece, packed)
    fold_row = lax.broadcasted_iota(jnp.int32, (own, points), 0)
    fold_col = lax.broadcasted_iota(jnp.int32, (own, points), 1)
    fold = jnp.where(fold_col // per_row == fold_row, 1.0, 0.0).astype(BF16)
    packed = times(fold, packed.astype(BF16))
    stored[:, : size_x * points] = totals
    lane = lax.broadcasted_iota(jnp.int32, (LANES, LANES), 1)
    for a in range(size_x):
        start = a * points // LANES * LANES
        shift = a * points - start
        found = stored[:, pl.ds(start, 2 * LANES)]
        if shift:
            found = pltpu.roll(found, 2 * LANES - shift, 1)
        found = jnp.where(lane < points, found[:, :LANES], 0.0)
        carried = jnp.where(place[0] == a, packed, 0.0)
        for g in range(size_z):
            sent[a * size_z + g] = (found[g * own : (g + 1) * own] + carried).astype(BF16)


def final_shares(sizes, place, arrived, block, colloc, shares, rows):
    size_x, _, per_rows = sizes
    pieces, height, lanes = shares.shape
    wide = height * lanes // (2 * per_rows)
    size_y = pieces // size_x
    part = colloc.shape[1] // size_y
    points = block.shape[0]
    own = size_x * per_rows
    per_row = points // own
    total = jnp.sum(arrived[...].astype(F32), axis=0)
    unfold_row = lax.broadcasted_iota(jnp.int32, (points, own), 0)
    unfold_col = lax.broadcasted_iota(jnp.int32, (points, own), 1)
    unfold = jnp.where(unfold_row // per_row == unfold_col, 1.0, 0.0).astype(BF16)
    spread_out = jnp.zeros((points, LANES), F32)
    for piece in in_pieces(total):
        spread_out += times(unfold, piece.astype(BF16))
    lane = lax.broadcasted_iota(jnp.int32, (points, LANES), 1)
    behind = W + PIECES * (lax.broadcasted_iota(jnp.int32, (points, LANES), 0) % per_row)
    kept = (lane >= behind) & (lane < behind + PIECES)
    potential = jnp.sum(jnp.where(kept, spread_out, 0.0), axis=1, keepdims=True)
    window = block[:, block.shape[1] - LANES :]
    pick = one_hot((own, LANES), lambda row: row + place[1] * own)
    weighted = (times(window, pick, 1, 1) * potential).astype(BF16)

    def spread(which):
        def target(row):
            inside = row % SUBLANES
            found = (row // SUBLANES) * per_rows + inside // 2
            return jnp.where((inside % 2 == which) & (inside // 2 < per_rows), found, -1)

        return one_hot((size_x * SUBLANES, own), target)

    left = times(spread(0), weighted, 1, 1) + times(spread(1), total[:, :points].astype(BF16))
    left = left.astype(BF16)
    width = colloc.shape[1]
    step = 4 * LANES
    for at in range(0, width, step):
        part_of = pl.ds(at, min(step, width - at))
        rows[:, part_of] = times(left, colloc[:, part_of])
    for c in range(size_y):
        start = c * part // LANES * LANES
        span = wide + LANES
        found = rows[:, pl.ds(start, span)]
        shift = c * part - start
        if shift:
            found = pltpu.roll(found, span - shift, 1)
        found = found[:, :wide].astype(BF16)
        for a in range(size_x):
            at = a * SUBLANES
            shares[a * size_y + c, :, :wide] = found[at : at + 4]
            for k in range(2):
                shares[a * size_y + c, 2 * k : 2 * k + 2, wide:] = found[
                    at + 4 : at + 6, k * LANES : (k + 1) * LANES
                ]


def outputs(arrived, coulomb, exchange):
    part = coulomb.shape[1]
    wide = arrived.shape[2] - LANES
    total = jnp.sum(arrived[...].astype(F32), axis=0)
    last = jnp.concatenate([total[:2, wide:], total[2:, wide:]], axis=1)
    for b, pair in enumerate((total[:2], total[2:], last)):
        coulomb[b : b + 1] = pair[:1, :part]
        exchange[b : b + 1] = pair[1:, :part]


def work(colloc, occ_coeffs, core):
    points, width = colloc.shape
    group = occ_coeffs.shape[1]
    size_x = lax.axis_size("gx")
    near_y = lax.axis_size("gy_1")
    size_y = lax.axis_size(GY)
    size_z = lax.axis_size("gz")
    row_count = core.shape[0]
    flat_cols = core.shape[2]
    per_rows = W // (size_x * size_z)
    own = size_x * per_rows
    part = width // size_y
    wide = -(-part // LANES) * LANES
    sizes = (size_x, size_z, per_rows)
    core_flat = core.reshape(row_count, flat_cols)
    place = jnp.stack([lax.axis_index("gx"), lax.axis_index("gz"), lax.axis_index("gy_0")])
    place = place.astype(jnp.int32)
    chunk = 10 * LANES
    steps = 4

    copies, block, sums = pl.pallas_call(
        functools.partial(occupied, sizes, chunk),
        in_specs=[IN_SMEM, IN_HBM, IN_HBM],
        out_specs=[IN_VMEM, IN_VMEM, IN_VMEM],
        out_shape=[
            jax.ShapeDtypeStruct((size_x, points, group), BF16),
            jax.ShapeDtypeStruct((points, group + LANES), BF16),
            jax.ShapeDtypeStruct((size_x, 2, LANES), BF16),
        ],
        scratch_shapes=[
            pltpu.VMEM((points, width), BF16),
            pltpu.VMEM((width, group), BF16),
            pltpu.SemaphoreType.DMA((2, steps)),
        ],
        compiler_params=pltpu.CompilerParams(vmem_limit_bytes=53 * 1024 * 1024),
        name="occupied",
    )(place, colloc, occ_coeffs)
    sums = exchange_pieces(sums, "gx")

    row_copies = pl.pallas_call(
        potential_rows,
        in_specs=[IN_VMEM, IN_VMEM, IN_VMEM],
        out_specs=IN_VMEM,
        out_shape=jax.ShapeDtypeStruct((near_y, points, group + LANES), BF16),
        scratch_shapes=[pltpu.VMEM((8, flat_cols), F32), pltpu.VMEM((row_count, LANES), F32)],
        compiler_params=PARAMS,
        name="potential_rows",
    )(sums, block, core_flat)
    near = exchange_pieces(row_copies, "gy_1")
    far = lax.ppermute(near, "gy_0", [(0, 1), (1, 0)])
    cols = exchange_pieces(copies, "gx")

    mark = pl.pallas_call(
        after,
        in_specs=[IN_VMEM],
        out_specs=IN_VMEM,
        out_shape=jax.ShapeDtypeStruct((SUBLANES, LANES), F32),
        compiler_params=PARAMS,
        name="after",
    )(cols)
    sent = pl.pallas_call(
        functools.partial(partial_totals, sizes, 8),
        in_specs=[IN_SMEM, IN_VMEM, IN_VMEM, IN_VMEM, IN_VMEM, IN_VMEM],
        out_specs=IN_VMEM,
        out_shape=jax.ShapeDtypeStruct((size_x * size_z, own, LANES), BF16),
        scratch_shapes=[pltpu.VMEM((LANES, flat_cols + LANES), F32)],
        compiler_params=PARAMS,
        name="partial_totals",
    )(place, mark, near, far, cols, core_flat)
    arrived = exchange_pieces(sent, ("gx", "gz"))

    shares = pl.pallas_call(
        functools.partial(final_shares, sizes),
        in_specs=[IN_SMEM, IN_VMEM, IN_VMEM, IN_VMEM],
        out_specs=IN_VMEM,
        out_shape=jax.ShapeDtypeStruct((size_x * size_y, 4, per_rows * wide // 2), BF16),
        scratch_shapes=[pltpu.VMEM((size_x * SUBLANES, (width // LANES + 2) * LANES), F32)],
        compiler_params=PARAMS,
        name="final_shares",
    )(place, arrived, block, colloc)
    arrived = exchange_pieces(shares, GX_GY)
    return pl.pallas_call(
        outputs,
        in_specs=[IN_VMEM],
        out_specs=[IN_VMEM, IN_VMEM],
        out_shape=[jax.ShapeDtypeStruct((per_rows, part), F32)] * 2,
        compiler_params=PARAMS,
        name="outputs",
    )(arrived)


def solution(mesh):
    split = Mesh(
        mesh.devices.reshape(mesh.shape["gx"], 2, 8, mesh.shape["gz"]), ("gx", "gy_0", "gy_1", "gz")
    )
    return jax.shard_map(
        work,
        mesh=split,
        in_specs=(P(GX_GY, None), P(None, "gz"), P("gx", GY, None)),
        out_specs=(P(("gx", "gz"), GY), P(("gx", "gz"), GY)),
        check_vma=False,
    )
```

```python
import functools

import jax
import jax.numpy as jnp
from jax import lax
from jax.experimental import pallas as pl
from jax.experimental.pallas import tpu as pltpu
from jax.sharding import Mesh
from jax.sharding import PartitionSpec as P

W = 96
LANES = 128
SUBLANES = 8
GRANT = 24 * 1024 * 1024
GY = ("gy_0", "gy_1")
GX_GY = ("gx", "gy_0", "gy_1")
BF16 = jnp.bfloat16
F32 = jnp.float32
IN_VMEM = pl.BlockSpec(memory_space=pltpu.VMEM)
IN_HBM = pl.BlockSpec(memory_space=pltpu.HBM)
IN_SMEM = pl.BlockSpec(memory_space=pltpu.SMEM)
PARAMS = pltpu.CompilerParams(vmem_limit_bytes=GRANT)


def exchange_pieces(pieces, axis):
    return lax.all_to_all(pieces, axis, split_axis=0, concat_axis=0, tiled=True)


def one_hot(shape, target):
    rows = lax.broadcasted_iota(jnp.int32, shape, 0)
    cols = lax.broadcasted_iota(jnp.int32, shape, 1)
    return jnp.where(cols == target(rows), 1.0, 0.0).astype(BF16)


def times(left, right, left_dim=1, right_dim=0):
    dims = (((left_dim,), (right_dim,)), ((), ()))
    return lax.dot_general(left, right, dims, preferred_element_type=F32)


PIECES = 2


def in_pieces(value):
    high = value.astype(BF16).astype(F32)
    return high, value - high


def occupied(sizes, chunk, _, colloc_hbm, coeffs_hbm, copies, block, sums, colloc, coeffs, sems):
    size_x, size_z, per_rows = sizes
    width, group = coeffs.shape
    points = colloc.shape[0]
    starts = [0, chunk, 2 * chunk, width // LANES * LANES - 3 * LANES]
    widths = [after_it - at for at, after_it in zip(starts, starts[1:] + [width])]
    copies_in = []
    for k, (at, size) in enumerate(zip(starts, widths)):
        part = pl.ds(at, size)
        copies_in.append(
            (
                pltpu.make_async_copy(colloc_hbm.at[:, part], colloc.at[:, part], sems.at[0, k]),
                pltpu.make_async_copy(coeffs_hbm.at[part, :], coeffs.at[part, :], sems.at[1, k]),
            )
        )
    for first, second in copies_in:
        first.start()
        second.start()
    own = size_x * per_rows

    def source(col):
        return ((col % own) // per_rows) * (size_z * per_rows) + (col // own) * per_rows + col % per_rows

    pick = one_hot((LANES, LANES), lambda rows: jnp.where(rows < W, source(rows), -1))
    acc = jnp.zeros((points, group), F32)
    for (first, second), at, size in zip(copies_in, starts, widths):
        first.wait()
        second.wait()
        part = pl.ds(at, size)
        acc += times(colloc[:, part], coeffs[part, :])
        if at == 0:
            block[:, group:] = times(colloc[:, :LANES], pick, 1, 1).astype(BF16)
    occ = acc.astype(BF16)
    vals = occ.astype(F32)
    ones = jnp.ones((SUBLANES, group), BF16)
    density = sum(times(ones, piece.astype(BF16), 1, 1) for piece in in_pieces(vals * vals))
    density = density[: sums.shape[1]].astype(BF16)
    block[:, :group] = occ
    for a in range(size_x):
        sums[a, :, :points] = density
        copies[a] = occ


def potential_rows(sums, block, core, copies, density, shares):
    size_x = sums.shape[0]
    size_y, points, _ = copies.shape
    group = block.shape[1] - LANES
    for a in range(size_x):
        density[:2, a * points : (a + 1) * points] = sums[a].astype(F32)[:, :points]
    right = jnp.broadcast_to(density[:1, :], (LANES, size_x * points)).astype(BF16)
    lane = lax.broadcasted_iota(jnp.int32, (points, LANES), 1)
    occ = block[:, :group]
    window = block[:, group:].astype(F32)
    halves = core.shape[0] // (size_y * points)
    for half in range(halves):
        at = half * size_y * points
        shares[pl.ds(at, size_y * points), :] = times(core[pl.ds(at, size_y * points), :], right, 1, 1)
    for y in range(size_y):
        tail = window
        for half in range(halves):
            share = shares[pl.ds((half * size_y + y) * points, points), :]
            for k, piece in enumerate(in_pieces(share)):
                tail = jnp.where(lane == W + PIECES * half + k, piece, tail)
        copies[y, :, :group] = occ
        copies[y, :, group:] = tail.astype(BF16)


def add_rows(per_step, rows, half, right, core, totals, tails):
    size_y, points, _ = rows.shape
    group = right.shape[1]
    height = per_step * points
    for y in range(0, size_y, per_step):
        left = rows[pl.ds(y, per_step), :, :group].reshape(height, group)
        tail = rows[pl.ds(y, per_step), :, group:].reshape(height, LANES)
        gram = times(left, right, 1, 1)
        at = pl.multiple_of(half * (size_y * points) + y * points, points)
        mixed = (core[pl.ds(at, height), :].astype(F32) * gram).astype(BF16)
        totals += times(tail, mixed, 0, 0)
        for step in range(per_step):
            tails += tail[step * points : (step + 1) * points].astype(F32)
    return totals, tails


def after(cols, mark):
    mark[...] = cols[0, :SUBLANES, :LANES].astype(F32)


def partial_totals(sizes, per_step, place, _, near, far, cols, core, sent, stored):
    size_x, size_z, per_rows = sizes
    points = far.shape[1]
    own = size_x * per_rows
    right = cols[...].reshape(-1, cols.shape[2])
    totals = jnp.zeros((LANES, right.shape[0]), F32)
    tails = jnp.zeros((points, LANES), F32)
    totals, tails = add_rows(per_step, near, place[2], right, core, totals, tails)
    totals, tails = add_rows(per_step, far, 1 - place[2], right, core, totals, tails)
    lane = lax.broadcasted_iota(jnp.int32, (points, LANES), 1)
    first = W + PIECES * place[2]
    kept = (lane >= first) & (lane < first + PIECES)
    share = jnp.sum(jnp.where(kept, tails, 0.0), axis=1, keepdims=True)
    per_row = points // own
    point = lax.broadcasted_iota(jnp.int32, (points, LANES), 0)
    behind = W + PIECES * (point % per_row)
    packed = jnp.zeros((points, LANES), F32)
    for k, piece in enumerate(in_pieces(share)):
        packed = jnp.where(lane == behind + k, piece, packed)
    fold_row = lax.broadcasted_iota(jnp.int32, (own, points), 0)
    fold_col = lax.broadcasted_iota(jnp.int32, (own, points), 1)
    fold = jnp.where(fold_col // per_row == fold_row, 1.0, 0.0).astype(BF16)
    packed = times(fold, packed.astype(BF16))
    stored[:, : size_x * points] = totals
    lane = lax.broadcasted_iota(jnp.int32, (LANES, LANES), 1)
    for a in range(size_x):
        start = a * points // LANES * LANES
        shift = a * points - start
        found = stored[:, pl.ds(start, 2 * LANES)]
        if shift:
            found = pltpu.roll(found, 2 * LANES - shift, 1)
        found = jnp.where(lane < points, found[:, :LANES], 0.0)
        carried = jnp.where(place[0] == a, packed, 0.0)
        for g in range(size_z):
            sent[a * size_z + g] = (found[g * own : (g + 1) * own] + carried).astype(BF16)


def final_shares(sizes, place, arrived, block, colloc, shares, rows):
    size_x, _, per_rows = sizes
    pieces, height, lanes = shares.shape
    wide = height * lanes // (2 * per_rows)
    size_y = pieces // size_x
    part = colloc.shape[1] // size_y
    points = block.shape[0]
    own = size_x * per_rows
    per_row = points // own
    total = jnp.sum(arrived[...].astype(F32), axis=0)
    unfold_row = lax.broadcasted_iota(jnp.int32, (points, own), 0)
    unfold_col = lax.broadcasted_iota(jnp.int32, (points, own), 1)
    unfold = jnp.where(unfold_row // per_row == unfold_col, 1.0, 0.0).astype(BF16)
    spread_out = jnp.zeros((points, LANES), F32)
    for piece in in_pieces(total):
        spread_out += times(unfold, piece.astype(BF16))
    lane = lax.broadcasted_iota(jnp.int32, (points, LANES), 1)
    behind = W + PIECES * (lax.broadcasted_iota(jnp.int32, (points, LANES), 0) % per_row)
    kept = (lane >= behind) & (lane < behind + PIECES)
    potential = jnp.sum(jnp.where(kept, spread_out, 0.0), axis=1, keepdims=True)
    window = block[:, block.shape[1] - LANES :]
    pick = one_hot((own, LANES), lambda row: row + place[1] * own)
    weighted = (times(window, pick, 1, 1) * potential).astype(BF16)

    def spread(which):
        def target(row):
            inside = row % SUBLANES
            found = (row // SUBLANES) * per_rows + inside // 2
            return jnp.where((inside % 2 == which) & (inside // 2 < per_rows), found, -1)

        return one_hot((size_x * SUBLANES, own), target)

    left = times(spread(0), weighted, 1, 1) + times(spread(1), total[:, :points].astype(BF16))
    left = left.astype(BF16)
    width = colloc.shape[1]
    step = 4 * LANES
    for at in range(0, width, step):
        part_of = pl.ds(at, min(step, width - at))
        rows[:, part_of] = times(left, colloc[:, part_of])
    for c in range(size_y):
        start = c * part // LANES * LANES
        span = wide + LANES
        found = rows[:, pl.ds(start, span)]
        shift = c * part - start
        if shift:
            found = pltpu.roll(found, span - shift, 1)
        found = found[:, :wide].astype(BF16)
        for a in range(size_x):
            at = a * SUBLANES
            shares[a * size_y + c, :, :wide] = found[at : at + 4]
            for k in range(2):
                shares[a * size_y + c, 2 * k : 2 * k + 2, wide:] = found[
                    at + 4 : at + 6, k * LANES : (k + 1) * LANES
                ]


def outputs(arrived, coulomb, exchange):
    part = coulomb.shape[1]
    wide = arrived.shape[2] - LANES
    total = jnp.sum(arrived[...].astype(F32), axis=0)
    last = jnp.concatenate([total[:2, wide:], total[2:, wide:]], axis=1)
    for b, pair in enumerate((total[:2], total[2:], last)):
        coulomb[b : b + 1] = pair[:1, :part]
        exchange[b : b + 1] = pair[1:, :part]


def work(colloc, occ_coeffs, core):
    points, width = colloc.shape
    group = occ_coeffs.shape[1]
    size_x = lax.axis_size("gx")
    near_y = lax.axis_size("gy_1")
    size_y = lax.axis_size(GY)
    size_z = lax.axis_size("gz")
    row_count = core.shape[0]
    flat_cols = core.shape[2]
    per_rows = W // (size_x * size_z)
    own = size_x * per_rows
    part = width // size_y
    wide = -(-part // LANES) * LANES
    sizes = (size_x, size_z, per_rows)
    core_flat = core.reshape(row_count, flat_cols)
    place = jnp.stack([lax.axis_index("gx"), lax.axis_index("gz"), lax.axis_index("gy_0")])
    place = place.astype(jnp.int32)
    chunk = 10 * LANES
    steps = 4

    copies, block, sums = pl.pallas_call(
        functools.partial(occupied, sizes, chunk),
        in_specs=[IN_SMEM, IN_HBM, IN_HBM],
        out_specs=[IN_VMEM, IN_VMEM, IN_VMEM],
        out_shape=[
            jax.ShapeDtypeStruct((size_x, points, group), BF16),
            jax.ShapeDtypeStruct((points, group + LANES), BF16),
            jax.ShapeDtypeStruct((size_x, 2, LANES), BF16),
        ],
        scratch_shapes=[
            pltpu.VMEM((points, width), BF16),
            pltpu.VMEM((width, group), BF16),
            pltpu.SemaphoreType.DMA((2, steps)),
        ],
        compiler_params=pltpu.CompilerParams(vmem_limit_bytes=53 * 1024 * 1024),
        name="occupied",
    )(place, colloc, occ_coeffs)
    sums = exchange_pieces(sums, "gx")

    row_copies = pl.pallas_call(
        potential_rows,
        in_specs=[IN_VMEM, IN_VMEM, IN_VMEM],
        out_specs=IN_VMEM,
        out_shape=jax.ShapeDtypeStruct((near_y, points, group + LANES), BF16),
        scratch_shapes=[pltpu.VMEM((8, flat_cols), F32), pltpu.VMEM((row_count, LANES), F32)],
        compiler_params=PARAMS,
        name="potential_rows",
    )(sums, block, core_flat)
    near = exchange_pieces(row_copies, "gy_1")
    far = lax.ppermute(near, "gy_0", [(0, 1), (1, 0)])
    cols = exchange_pieces(copies, "gx")

    mark = pl.pallas_call(
        after,
        in_specs=[IN_VMEM],
        out_specs=IN_VMEM,
        out_shape=jax.ShapeDtypeStruct((SUBLANES, LANES), F32),
        compiler_params=PARAMS,
        name="after",
    )(cols)
    sent = pl.pallas_call(
        functools.partial(partial_totals, sizes, 8),
        in_specs=[IN_SMEM, IN_VMEM, IN_VMEM, IN_VMEM, IN_VMEM, IN_VMEM],
        out_specs=IN_VMEM,
        out_shape=jax.ShapeDtypeStruct((size_x * size_z, own, LANES), BF16),
        scratch_shapes=[pltpu.VMEM((LANES, flat_cols + LANES), F32)],
        compiler_params=PARAMS,
        name="partial_totals",
    )(place, mark, near, far, cols, core_flat)
    arrived = exchange_pieces(sent, ("gx", "gz"))

    shares = pl.pallas_call(
        functools.partial(final_shares, sizes),
        in_specs=[IN_SMEM, IN_VMEM, IN_VMEM, IN_VMEM],
        out_specs=IN_VMEM,
        out_shape=jax.ShapeDtypeStruct((size_x * size_y, 4, per_rows * wide // 2), BF16),
        scratch_shapes=[pltpu.VMEM((size_x * SUBLANES, (width // LANES + 2) * LANES), F32)],
        compiler_params=PARAMS,
        name="final_shares",
    )(place, arrived, block, colloc)
    arrived = exchange_pieces(shares, GX_GY)
    return pl.pallas_call(
        outputs,
        in_specs=[IN_VMEM],
        out_specs=[IN_VMEM, IN_VMEM],
        out_shape=[jax.ShapeDtypeStruct((per_rows, part), F32)] * 2,
        compiler_params=PARAMS,
        name="outputs",
    )(arrived)


def solution(mesh):
    split = Mesh(
        mesh.devices.reshape(mesh.shape["gx"], 2, 8, mesh.shape["gz"]), ("gx", "gy_0", "gy_1", "gz")
    )
    return jax.shard_map(
        work,
        mesh=split,
        in_specs=(P(GX_GY, None), P(None, "gz"), P("gx", GY, None)),
        out_specs=(P(("gx", "gz"), GY), P(("gx", "gz"), GY)),
        check_vma=False,
    )
```
